128 devices in a mesh: row: 8 (over y, core), col: 16 (over z, x).
Axes of the slice: x: 4, y: 4, z: 4, core: 2. Of those that a mesh axis runs over, the one named last changes fastest.
Arguments:
- blocks: float32 [32768, 128, 128], P(('row', 'col')), may hold values from -0.25 to 0.25
- block_rows: int32 [128, 256], P(('row', 'col')), may hold values from 0 to 2047, as said below
- block_cols: int32 [128, 256], P(('row', 'col')), may hold values from 0 to 1023
- diagonal: float32 [2097152], P(('row', 'col')), may hold values from 1 to 4
- right_sides: float32 [2, 2097152], P(None, ('row', 'col')), may hold values from -6 to 6
Outputs:
- solution: float32 [2, 2097152], P(None, ('row', 'col'))
- hessenberg: float32 [2, 9, 8], replicated
The draws below stay inside these ranges and needn't reach their ends.
Inputs may be any that keep to these rules, and one draw needn't show every extreme that they name: `block_rows`: non-decreasing along each tile's slots; a local block row may hold no stored block.
All inputs are finite; a program needn't handle non-finite values.
Results may differ from the reference program's by a relative error of at most 0.0085.
Values sent between devices are 32-bit elements; how exact they have to be, the bound alone decides.
No kernel may reach another device: no remote copies, remote signals or barrier semaphores. Data moves between devices by JAX's collectives and lax.ppermute only.
A program may use at most 128 MiB of HBM per device.

```python
import math
import jax
import jax.numpy as jnp
from jax import lax

BS = 128
PB = 128
NRHS = 2
STEPS = 8
TILES = 128
ROWB = 2048
COLB = 1024
CAP = 256
NUNK = 2097152
N_ROW = 8
N_COL = 16


def draw_block_rows(key, part):
    levels_top = ROWB.bit_length() - 1
    level_key = jax.random.fold_in(key, 11)
    value_key = jax.random.fold_in(key, 12)
    order_key = jax.random.fold_in(key, 13)
    levels = jax.random.randint(level_key, (TILES, CAP), 0, levels_top + 1, dtype=jnp.int32)
    spans = jnp.left_shift(jnp.ones_like(levels), levels)
    raw = jax.random.randint(value_key, (TILES, CAP), 0, spans, dtype=jnp.int32)
    order = jax.random.permutation(order_key, ROWB).astype(jnp.int32)
    placed = jnp.take(order, raw)
    return jnp.sort(placed, axis=1).astype(jnp.int32)


def place_ends(entries, key, low, high):
    index_at = [jax.random.randint(jax.random.fold_in(key, axis), (), 0, length) for axis, length in enumerate(entries.shape)]
    longest = entries.shape.index(max(entries.shape))
    beside = index_at[:longest] + [(index_at[longest] + 1) % entries.shape[longest]] + index_at[longest + 1:]
    return entries.at[tuple(index_at)].set(low).at[tuple(beside)].set(high)


def block_scale(key, dims, split, low, largest):
    loudness = 1.0
    for axis_at, blocks in split:
        heights = jax.random.uniform(jax.random.fold_in(jax.random.fold_in(key, 6), axis_at), (blocks,), jnp.float32, low / len(split), largest / len(split))
        loudness = loudness * jnp.repeat(jnp.exp(heights), dims[axis_at] // blocks).reshape((-1,) + (1,) * (len(dims) - 1 - axis_at))
    return loudness


def bell_draw(key, extent, width, reach, shards=(), held_as=jnp.bfloat16):
    array = width * jax.random.normal(key, extent, jnp.float32)
    if shards:
        array = array * block_scale(key, extent, shards, -0.22, 0.18)
    return jnp.clip(array, -reach, reach).astype(held_as)


def setup_inputs(seed: int = 0) -> dict:
    key_of = jax.random.split(jax.random.key(seed), 6)
    blocks = bell_draw(key_of[0], (TILES * CAP, BS, BS), (4 * BS) ** -0.5, 0.25, ((0, 128),), jnp.float32)
    block_rows = draw_block_rows(jax.random.fold_in(key_of[5], 71), 0)
    block_cols = place_ends(jax.random.randint(key_of[2], (TILES, CAP), 0, COLB), jax.random.fold_in(key_of[2], 1), 0, COLB - 1).astype(jnp.int32)
    diagonal = jnp.clip(jnp.exp(math.log(4.0) - 1.3862944 * jax.random.uniform(key_of[3], (NUNK,), jnp.float32) ** block_scale(key_of[3], (NUNK,), ((0, 128),), -0.2, 0.2)), 1.0, 4.0)
    right_sides = bell_draw(key_of[4], (NRHS, NUNK), 1.0, 6.0, ((1, 128),), jnp.float32)
    return dict(blocks=blocks, block_rows=block_rows, block_cols=block_cols, diagonal=diagonal, right_sides=right_sides)


epsilon = 1e-06

def least_squares(hessenberg, initial_norm):
    total_steps = hessenberg.shape[2]
    targets = [initial_norm] + [jnp.zeros_like(initial_norm) for j in range(total_steps)]
    cosines, sines, triangle = ([], [], [])
    for j in range(total_steps):
        column = [hessenberg[:, i, j] for i in range(j + 2)]
        for i in range(j):
            leading, trailing = (column[i], column[i + 1])
            column[i] = cosines[i] * leading + sines[i] * trailing
            column[i + 1] = cosines[i] * trailing - sines[i] * leading
        radius = jnp.sqrt(column[j] * column[j] + column[j + 1] * column[j + 1])
        cosine = column[j] / radius
        sine_term = column[j + 1] / radius
        column[j] = radius
        cosines.append(cosine)
        sines.append(sine_term)
        targets[j + 1] = -sine_term * targets[j]
        targets[j] = cosine * targets[j]
        triangle.append(column[:j + 1])
    coeffs = [None] * total_steps
    for j in reversed(range(total_steps)):
        running = targets[j]
        for k in range(j + 1, total_steps):
            running = running - triangle[k][j] * coeffs[k]
        coeffs[j] = running / triangle[j][j]
    return jnp.stack(coeffs, axis=1)

def apply_matrix(vector, blocks, block_rows, block_cols, diagonal):
    systems = vector.shape[0]
    pieces = vector.reshape(systems, N_ROW, N_COL, PB * BS)
    tiled = blocks.reshape(TILES, CAP, BS, BS)

    def one_tile(accumulated, tile_index):
        row_index = tile_index // N_COL
        col_index = tile_index % N_COL
        column_group = lax.dynamic_index_in_dim(pieces, col_index, 2, keepdims=False)
        column_group = column_group.reshape(systems, N_ROW * PB, BS)
        picked = jnp.take(column_group, block_cols[tile_index].astype(jnp.int32), axis=1)
        tile_blocks = lax.dynamic_index_in_dim(tiled, tile_index, 0, keepdims=False)
        products = jnp.einsum('kij,nkj->nki', tile_blocks, picked, precision=lax.Precision.HIGHEST)
        row_sums = jax.ops.segment_sum(jnp.transpose(products, (1, 0, 2)), block_rows[tile_index].astype(jnp.int32), num_segments=N_COL * PB)
        partial_value = jnp.transpose(row_sums, (1, 0, 2)).reshape(systems, N_COL * PB * BS)
        accumulated = accumulated.at[:, row_index].add(partial_value)
        return (accumulated, None)
    start = jnp.zeros((systems, N_ROW, N_COL * PB * BS), jnp.float32)
    accumulated, unused = lax.scan(one_tile, start, jnp.arange(TILES, dtype=jnp.int32))
    return diagonal[None, :] * vector + accumulated.reshape(systems, -1)

def reference(blocks, block_rows, block_cols, diagonal, right_sides):
    systems = right_sides.shape[0]
    initial_norm = jnp.sqrt(lax.optimization_barrier(jnp.sum(right_sides * right_sides, axis=1)) + epsilon)
    krylov_basis = [right_sides / initial_norm[:, None]]
    hessenberg = jnp.zeros((systems, STEPS + 1, STEPS), jnp.float32)
    for j in range(STEPS):
        candidate = apply_matrix(krylov_basis[j], blocks, block_rows, block_cols, diagonal)
        stacked = jnp.stack(krylov_basis)
        coeffs = jnp.einsum('inl,nl->ni', stacked, candidate, precision=lax.Precision.HIGHEST)
        candidate = candidate - jnp.einsum('ni,inl->nl', coeffs, stacked, precision=lax.Precision.HIGHEST)
        new_norm = jnp.sqrt(lax.optimization_barrier(jnp.sum(candidate * candidate, axis=1)) + epsilon)
        hessenberg = hessenberg.at[:, :j + 1, j].set(coeffs)
        hessenberg = hessenberg.at[:, j + 1, j].set(new_norm)
        krylov_basis.append(candidate / new_norm[:, None])
    weights = least_squares(hessenberg, initial_norm)
    solution = jnp.einsum('ni,inl->nl', weights, jnp.stack(krylov_basis[:STEPS]), precision=lax.Precision.HIGHEST)
    return (solution, hessenberg)
```

```python
import functools

import jax
import jax.numpy as jnp
from jax import lax
from jax.experimental import pallas as pl
from jax.experimental.pallas import tpu as pltpu
from jax.sharding import PartitionSpec as P

STEPS = 8
BS = 128
SRC_SLOTS = 56
DST_SLOTS = 24
ROW = "row"
COL = "col"
BOTH = ("row", "col")
F32 = jnp.float32
BF16 = jnp.bfloat16

epsilon = 1e-06

QQ, PP, GRAM, FLAG = 9, 10, 16, 127


def swap(value, axis):
    return lax.all_to_all(value, axis, split_axis=0, concat_axis=0, tiled=True)


def least_squares(hessenberg, initial_norm):
    total_steps = hessenberg.shape[2]
    targets = [initial_norm] + [jnp.zeros_like(initial_norm) for j in range(total_steps)]
    cosines, sines, triangle = ([], [], [])
    for j in range(total_steps):
        column = [hessenberg[:, i, j] for i in range(j + 2)]
        rotate(column, cosines, sines, targets, triangle)
    return jnp.stack(back_substitute(triangle, targets), axis=1)


def rotate(column, cosines, sines, targets, triangle):
    j = len(column) - 2
    for i in range(j):
        leading, trailing = (column[i], column[i + 1])
        column[i] = cosines[i] * leading + sines[i] * trailing
        column[i + 1] = cosines[i] * trailing - sines[i] * leading
    radius = jnp.sqrt(column[j] * column[j] + column[j + 1] * column[j + 1])
    cosine = column[j] / radius
    sine_term = column[j + 1] / radius
    column[j] = radius
    cosines.append(cosine)
    sines.append(sine_term)
    targets[j + 1] = -sine_term * targets[j]
    targets[j] = cosine * targets[j]
    triangle.append(column[: j + 1])


def back_substitute(triangle, targets):
    total_steps = len(triangle)
    coeffs = [None] * total_steps
    for j in reversed(range(total_steps)):
        running = targets[j]
        for k in range(j + 1, total_steps):
            running = running - triangle[k][j] * coeffs[k]
        coeffs[j] = running / triangle[j][j]
    return coeffs


def dense_cycle(blocks, block_rows, block_cols, diagonal, right_sides):
    systems = right_sides.shape[0]
    groups = lax.axis_size(COL)
    length = right_sides.shape[1]
    row_count = groups * (length // BS)
    positions = jnp.arange(row_count, dtype=jnp.int32)
    onehot = (block_rows[0][None, :] == positions[:, None]).astype(F32)
    high = lax.Precision.HIGHEST

    def everywhere(value):
        return lax.psum(lax.psum(value, ROW), COL)

    def apply_matrix(vector):
        copies = jnp.broadcast_to(vector, (lax.axis_size(ROW), *vector.shape))
        gathered = jnp.moveaxis(swap(copies, ROW), 0, 1).reshape(systems, -1, BS)
        picked = jnp.take(gathered, block_cols[0], axis=1)
        products = jnp.einsum("kij,nkj->nki", blocks, picked, precision=high)
        partial = jnp.einsum("mk,nki->mni", onehot, products, precision=high)
        own = swap(partial.reshape(groups, -1, systems, BS), COL).sum(axis=0)
        return diagonal[None, :] * vector + jnp.transpose(own, (1, 0, 2)).reshape(systems, -1)

    def norm(vector):
        return jnp.sqrt(everywhere(jnp.sum(vector * vector, axis=1)) + epsilon)

    initial_norm = norm(right_sides)
    basis = jnp.zeros((STEPS + 1, systems, length), F32).at[0].set(right_sides / initial_norm[:, None])
    hessenberg = jnp.zeros((systems, STEPS + 1, STEPS), F32)

    def step(j, state):
        basis, hessenberg = state
        candidate = apply_matrix(basis[j])
        coeffs = everywhere(jnp.einsum("inl,nl->ni", basis, candidate, precision=high))
        candidate = candidate - jnp.einsum("ni,inl->nl", coeffs, basis, precision=high)
        new_norm = norm(candidate)
        below = (jnp.arange(STEPS + 1) == j + 1).astype(F32)
        column = coeffs + below[None, :] * new_norm[:, None]
        here = (jnp.arange(STEPS) == j).astype(F32)
        hessenberg = hessenberg + column[:, :, None] * here[None, None, :]
        basis = basis.at[j + 1].set(candidate / new_norm[:, None])
        return basis, hessenberg

    basis, hessenberg = lax.fori_loop(0, STEPS, step, (basis, hessenberg))
    weights = least_squares(hessenberg, initial_norm)
    solution = jnp.einsum("ni,inl->nl", weights, basis[:STEPS], precision=high)
    return solution, hessenberg


def whole(count):
    return [pl.BlockSpec(memory_space=pltpu.VMEM)] * count


def call(kernel, outs, operands, scratch=(), vmem=24 << 20, name=None):
    return pl.pallas_call(
        kernel,
        out_shape=outs,
        in_specs=whole(len(operands)),
        out_specs=jax.tree.map(lambda o: pl.BlockSpec(memory_space=pltpu.VMEM), outs),
        scratch_shapes=list(scratch),
        compiler_params=pltpu.CompilerParams(vmem_limit_bytes=vmem),
        name=name,
    )(*operands)


def pieces(value, count):
    out = []
    for _ in range(count):
        piece = value.astype(BF16)
        out.append(piece)
        value = value - piece.astype(F32)
    return out


def pick(selector, value, count=3):
    return sum(jnp.dot(selector, piece, preferred_element_type=F32) for piece in pieces(value, count))


def turn_kernel(blocks_ref, turned_ref):
    for pair in range(turned_ref.shape[0]):
        for half in range(2):
            turned_ref[pair, :, half * BS : (half + 1) * BS] = blocks_ref[2 * pair + half].T.astype(BF16)


def turn_blocks(blocks, per_step=16):
    count = blocks.shape[0]
    return pl.pallas_call(
        turn_kernel,
        out_shape=jax.ShapeDtypeStruct((count // 2, BS, 2 * BS), BF16),
        grid=(count // per_step,),
        in_specs=[pl.BlockSpec((per_step, BS, BS), lambda i: (i, 0, 0))],
        out_specs=pl.BlockSpec((per_step // 2, BS, 2 * BS), lambda i: (i, 0, 0)),
        compiler_params=pltpu.CompilerParams(vmem_limit_bytes=8 << 20),
        name="turn_blocks",
    )(blocks)


def product_kernel(extra, *refs):
    if extra:
        got_ref, spread_ref, turned_ref, sums_ref, extra_ref, out_ref, left_ref, prod_ref = refs
    else:
        got_ref, spread_ref, turned_ref, sums_ref, out_ref, left_ref, prod_ref = refs
    sources, slots = got_ref.shape[0], got_ref.shape[1]
    targets, target_slots = out_ref.shape[0], out_ref.shape[1]
    got = got_ref[...].reshape(sources * slots, 2 * BS)
    count = spread_ref.shape[0]
    for at, piece in enumerate(pieces(got, 2)):
        picked = jnp.dot(spread_ref[...], piece, preferred_element_type=F32)
        left_ref[pl.ds(2 * at, count, stride=4), :] = picked[:, :BS]
        left_ref[pl.ds(2 * at + 1, count, stride=4), :] = picked[:, BS:]
    first = lax.broadcasted_iota(jnp.int32, (8, BS), 0) < 4

    def pair_step(pair, carry):
        rows = pl.ds(pl.multiple_of(8 * pair, 8), 8)
        both = jnp.dot(left_ref[rows, :].astype(BF16), turned_ref[pair], preferred_element_type=F32)
        prod_ref[rows, :] = jnp.where(first, both[:, :BS], both[:, BS:])
        return carry

    lax.fori_loop(0, turned_ref.shape[0], pair_step, 0, unroll=16)
    products = jnp.concatenate(
        [prod_ref[pl.ds(n, count, stride=4), :] + prod_ref[pl.ds(n + 2, count, stride=4), :] for n in range(2)],
        axis=1,
    )
    summed = pick(sums_ref[...], products)
    out_ref[...] = summed.reshape(targets, target_slots, 2 * BS)
    ride = got_ref[0, slots - 1 : slots, :]
    for s in range(1, sources):
        ride = ride + got_ref[s, slots - 1 : slots, :]
    for t in range(targets):
        row = ride + extra_ref[t : t + 1, :] if extra else ride
        out_ref[t, target_slots - 1 : target_slots, :] = row


def block_products(got, spread, turned, sums, extra=None):
    operands = (got, spread, turned, sums) + ((extra,) if extra is not None else ())
    count = spread.shape[0]
    targets = sums.shape[0] // DST_SLOTS
    return call(
        functools.partial(product_kernel, extra is not None),
        jax.ShapeDtypeStruct((targets, DST_SLOTS, 2 * BS), F32),
        operands,
        [pltpu.VMEM((4 * count, BS), F32), pltpu.VMEM((4 * count, BS), F32)],
        vmem=16 << 20,
        name="block_products",
    )


def lane_of(row, lane):
    return row[:, lane : lane + 1]


def total(value):
    return jnp.sum(value, axis=0, keepdims=True)


def send_out(values, wanted_ref, ride, out_ref):
    out = pick(wanted_ref[...], values)
    out_ref[...] = out.reshape(out_ref.shape)
    slots = out_ref.shape[1]
    for s in range(out_ref.shape[0]):
        out_ref[s, slots - 1 : slots, :] = ride


def start_kernel(b_ref, wanted_ref, ride_ref, out_ref):
    values = jnp.concatenate([b_ref[0], b_ref[1]], axis=1)
    send_out(values, wanted_ref, ride_ref[0:1, :], out_ref)


def inner_products(dots_ref, vs, q, p, j):
    rides = []
    for n in range(2):
        cut = slice(n * BS, (n + 1) * BS)
        dots_ref[...] = jnp.zeros(dots_ref.shape, F32)
        qn, pn = q[:, cut], p[:, cut]
        for i in range(j):
            vn = vs[i][:, cut]
            dots_ref[i : i + 1, :] = total(vn * pn)
            dots_ref[GRAM + i : GRAM + i + 1, :] = total(vn * qn)
        dots_ref[j : j + 1, :] = total(qn * pn)
        dots_ref[QQ : QQ + 1, :] = total(qn * qn)
        dots_ref[PP : PP + 1, :] = total(pn * pn)
        ones = jnp.ones((8, BS), F32)
        row = lax.dot_general(
            ones, dots_ref[...], (((1,), (1,)), ((), ())),
            precision=lax.Precision.HIGHEST, preferred_element_type=F32,
        )
        rides.append(row[0:1, :])
    return jnp.concatenate(rides, axis=1)


def arrived(got_ref, scatter_ref):
    flat = got_ref[...].reshape(-1, 2 * BS)
    return pick(scatter_ref[...], flat)


def ridden(got_ref):
    slots = got_ref.shape[1]
    ride = got_ref[0, slots - 1 : slots, :]
    for s in range(1, got_ref.shape[0]):
        ride = ride + got_ref[s, slots - 1 : slots, :]
    return ride


def side_by_side(ref):
    return jnp.concatenate([ref[0], ref[1]], axis=1)


def first_kernel(got_ref, scatter_ref, b_ref, diag_ref, wanted_ref, p_ref, q_ref, out_ref, dots_ref):
    b = side_by_side(b_ref)
    p = arrived(got_ref, scatter_ref) + jnp.concatenate([diag_ref[...]] * 2, axis=1) * b
    p_ref[...] = p
    q_ref[...] = b
    send_out(p, wanted_ref, inner_products(dots_ref, [], b, p, 0), out_ref)


def column_of(ride, j):
    lane = lax.broadcasted_iota(jnp.int32, (1, BS), 1)
    out = []
    for n in range(2):
        row = ride[:, n * BS : (n + 1) * BS]
        inverse = 1.0 / jnp.sqrt(lane_of(row, QQ) + epsilon)
        h = row * jnp.where(lane == j, inverse * inverse, jnp.broadcast_to(inverse, (1, BS)))
        out.append((h, inverse))
    return out


def step_kernel(j, *refs):
    got_ref, scatter_ref, q_ref, p_ref, diag_ref, wanted_ref = refs[:6]
    v_refs = refs[6 : 6 + j]
    m_refs = refs[6 + j : 6 + 2 * j]
    v_ref, m_ref, q_out, p_out, ride_out, out_ref, dots_ref = refs[6 + 2 * j :]
    ride = ridden(got_ref)
    ride_out[...] = jnp.broadcast_to(ride, ride_out.shape)
    coeffs = column_of(ride, j)
    z = arrived(got_ref, scatter_ref)
    for n, (h, inverse) in enumerate(coeffs):
        cut = slice(n * BS, (n + 1) * BS)
        pn = p_ref[:, cut]
        v = q_ref[:, cut] * inverse
        m = pn * inverse
        v_ref[:, cut] = v
        m_ref[:, cut] = m
        q_next = m - lane_of(h, j) * v
        p_next = (z[:, cut] + diag_ref[...] * pn) * inverse - lane_of(h, j) * m
        for i in range(j):
            q_next = q_next - lane_of(h, i) * v_refs[i][:, cut]
            p_next = p_next - lane_of(h, i) * m_refs[i][:, cut]
        q_out[:, cut] = q_next
        p_out[:, cut] = p_next
    p = p_out[...]
    ride = inner_products(dots_ref, [r[...] for r in v_refs] + [v_ref[...]], q_out[...], p, j + 1)
    if j + 1 == STEPS - 1:
        out_ref[...] = jnp.broadcast_to(ride[:, None, :], out_ref.shape)
    else:
        send_out(p, wanted_ref, ride, out_ref)


def finish_kernel(*refs):
    last_ref = refs[0]
    ride_refs = refs[1:STEPS]
    q_ref = refs[STEPS]
    v_refs = refs[STEPS + 1 : 2 * STEPS]
    solution_ref, hessenberg_ref = refs[2 * STEPS :]
    last = jnp.sum(last_ref[...], axis=0)
    rides = [r[0:1, :] for r in ride_refs] + [last]
    per_step = [column_of(ride, j) for j, ride in enumerate(rides)]
    lane = lax.broadcasted_iota(jnp.int32, (1, BS), 1)
    for n in range(2):
        rows = [ride[:, n * BS : (n + 1) * BS] for ride in rides]
        norms = [jnp.sqrt(lane_of(row, QQ) + epsilon) for row in rows]
        columns = [[lane_of(per_step[j][n][0], i) for i in range(j + 1)] for j in range(STEPS)]
        inverses = [per_step[j][n][1] for j in range(STEPS)]
        h = columns[-1]
        remainder = lane_of(rows[-1], PP) * inverses[-1] * inverses[-1]
        for i in range(STEPS):
            remainder = remainder - 2.0 * h[i] * h[i]
            own = lane_of(rows[i], QQ) * inverses[i] * inverses[i]
            remainder = remainder + h[i] * h[i] * own
            for k in range(i):
                gram = lane_of(rows[i], GRAM + k) * inverses[i]
                remainder = remainder + 2.0 * h[i] * h[k] * gram
        final_norm = jnp.sqrt(jnp.maximum(remainder, 0.0) + epsilon)
        below = norms[1:] + [final_norm]
        full = []
        for j in range(STEPS):
            row = jnp.where(lane <= j, per_step[j][n][0], 0.0)
            full.append(jnp.where(lane == j + 1, below[j], row))
        hessenberg_ref[n] = jnp.concatenate(full, axis=0)
        targets = [norms[0]] + [jnp.zeros_like(norms[0])] * STEPS
        cosines, sines, triangle = [], [], []
        for j in range(STEPS):
            rotate(columns[j] + [below[j]], cosines, sines, targets, triangle)
        weights = back_substitute(triangle, targets)
        cut = slice(n * BS, (n + 1) * BS)
        acc = (weights[-1] * inverses[-1]) * q_ref[:, cut]
        for i in range(STEPS - 1):
            acc = acc + weights[i] * v_refs[i][:, cut]
        solution_ref[n] = acc


def slots_of(index, groups, slots, usable):
    places = jnp.arange(groups * BS, dtype=jnp.int32)
    hits = index[:, None] == places[None, :]
    present = hits.any(axis=0).astype(F32).reshape(groups, BS)
    lane = jnp.arange(BS, dtype=jnp.int32)
    before = (lane[:, None] < lane[None, :]).astype(F32)
    rank = jnp.dot(present, before)
    largest = jnp.max(jnp.sum(present, axis=1))
    slot = rank + (jnp.arange(groups, dtype=F32) * slots)[:, None]
    slot_of_block = jnp.sum(jnp.where(hits, slot.reshape(-1)[None, :], 0.0), axis=1)
    wide = jnp.arange(BS, dtype=F32)
    match = (rank[:, None, :] == wide[None, :, None]) & (present[:, None, :] > 0)
    listed = jnp.sum(jnp.where(match, wide[None, None, :] + 1.0, 0.0), axis=2) - 1.0
    listed = jnp.where(wide[None, :] < usable, listed, -1.0)
    return slot_of_block, listed, largest


def body(blocks, block_rows, block_cols, diagonal, right_sides):
    rows_n, cols_n = lax.axis_size(ROW), lax.axis_size(COL)
    count = blocks.shape[0]
    b = right_sides.reshape(2, -1, BS)
    diag = diagonal.reshape(-1, BS)
    block_at = jnp.arange(BS, dtype=F32)

    src_slot, src_list, src_most = slots_of(block_cols[0], rows_n, SRC_SLOTS, SRC_SLOTS - 1)
    asked = swap(jnp.broadcast_to(src_list[:, None, :], (rows_n, 8, BS)), ROW)
    turned = turn_blocks(blocks)
    dst_slot, dst_list, dst_most = slots_of(block_rows[0], cols_n, DST_SLOTS, DST_SLOTS - 1)
    over = ((src_most > SRC_SLOTS - 1) | (dst_most > DST_SLOTS - 1)).astype(F32)
    spread = (src_slot[:, None] == jnp.arange(rows_n * SRC_SLOTS, dtype=F32)[None, :]).astype(BF16)
    sums = (dst_slot[None, :] == jnp.arange(cols_n * DST_SLOTS, dtype=F32)[:, None]).astype(BF16)
    wanted = (asked[:, 0, :SRC_SLOTS].reshape(-1)[:, None] == block_at[None, :]).astype(BF16)
    extra = jnp.concatenate([dst_list, jnp.zeros_like(dst_list)], axis=1)
    lanes = jnp.arange(2 * BS)
    ride = jnp.where(lanes[None, :] == BS + FLAG, over, 0.0) + jnp.zeros((8, 1), F32)

    out_shape = jax.ShapeDtypeStruct((rows_n, SRC_SLOTS, 2 * BS), F32)
    vec = jax.ShapeDtypeStruct((BS, 2 * BS), F32)
    dots = pltpu.VMEM((BS, BS), F32)

    send = call(start_kernel, out_shape, (b, wanted, ride), name="start")
    partial = block_products(swap(send, ROW), spread, turned, sums, extra)
    got = swap(partial, COL)
    last_row = got[:, DST_SLOTS - 1, :]
    overflow = jnp.sum(last_row[:, BS + FLAG])
    scatter = (last_row[:, :DST_SLOTS].reshape(-1)[None, :] == block_at[:, None]).astype(BF16)
    p, q, send = call(first_kernel, (vec, vec, out_shape), (got, scatter, b, diag, wanted), [dots], name="first")
    vs, ms, rides = [], [], []
    for j in range(STEPS - 1):
        got = swap(block_products(swap(send, ROW), spread, turned, sums), COL)
        last = j + 1 == STEPS - 1
        outs = (
            vec, vec, vec, vec, jax.ShapeDtypeStruct((8, 2 * BS), F32),
            jax.ShapeDtypeStruct((rows_n * cols_n, 1, 2 * BS), F32) if last else out_shape,
        )
        v, m, q, p, ride, send = call(
            functools.partial(step_kernel, j), outs, (got, scatter, q, p, diag, wanted, *vs, *ms), [dots],
            name=f"step_{j}",
        )
        vs.append(v)
        ms.append(m)
        rides.append(ride)
    final = swap(send, BOTH)
    solution, hessenberg = call(
        finish_kernel,
        (jax.ShapeDtypeStruct((2, BS, BS), F32), jax.ShapeDtypeStruct((2, STEPS, BS), F32)),
        (final, *rides, q, *vs),
        name="finish",
    )
    solution = solution.reshape(2, -1)
    hessenberg = jnp.swapaxes(hessenberg[:, :, : STEPS + 1], 1, 2)
    return lax.cond(
        overflow > 0.0,
        dense_cycle,
        lambda *unused: (solution, hessenberg),
        blocks, block_rows, block_cols, diagonal, right_sides,
    )


def solution(mesh):
    placed = (P(BOTH, None, None), P(BOTH, None), P(BOTH, None), P(BOTH), P(None, BOTH))
    return jax.shard_map(
        body, mesh=mesh, in_specs=placed, out_specs=(P(None, BOTH), P()), check_vma=False
    )
```

```python
import functools

import jax
import jax.numpy as jnp
from jax import lax
from jax.experimental import pallas as pl
from jax.experimental.pallas import tpu as pltpu
from jax.sharding import PartitionSpec as P

STEPS = 8
BS = 128
SRC_SLOTS = 56
DST_SLOTS = 24
ROW = "row"
COL = "col"
BOTH = ("row", "col")
F32 = jnp.float32
BF16 = jnp.bfloat16

epsilon = 1e-06

QQ, PP, GRAM, FLAG = 9, 10, 16, 127


def swap(value, axis):
    return lax.all_to_all(value, axis, split_axis=0, concat_axis=0, tiled=True)


def least_squares(hessenberg, initial_norm):
    total_steps = hessenberg.shape[2]
    targets = [initial_norm] + [jnp.zeros_like(initial_norm) for j in range(total_steps)]
    cosines, sines, triangle = ([], [], [])
    for j in range(total_steps):
        column = [hessenberg[:, i, j] for i in range(j + 2)]
        rotate(column, cosines, sines, targets, triangle)
    return jnp.stack(back_substitute(triangle, targets), axis=1)


def rotate(column, cosines, sines, targets, triangle):
    j = len(column) - 2
    for i in range(j):
        leading, trailing = (column[i], column[i + 1])
        column[i] = cosines[i] * leading + sines[i] * trailing
        column[i + 1] = cosines[i] * trailing - sines[i] * leading
    radius = jnp.sqrt(column[j] * column[j] + column[j + 1] * column[j + 1])
    cosine = column[j] / radius
    sine_term = column[j + 1] / radius
    column[j] = radius
    cosines.append(cosine)
    sines.append(sine_term)
    targets[j + 1] = -sine_term * targets[j]
    targets[j] = cosine * targets[j]
    triangle.append(column[: j + 1])


def back_substitute(triangle, targets):
    total_steps = len(triangle)
    coeffs = [None] * total_steps
    for j in reversed(range(total_steps)):
        running = targets[j]
        for k in range(j + 1, total_steps):
            running = running - triangle[k][j] * coeffs[k]
        coeffs[j] = running / triangle[j][j]
    return coeffs


def dense_cycle(blocks, block_rows, block_cols, diagonal, right_sides):
    systems = right_sides.shape[0]
    groups = lax.axis_size(COL)
    length = right_sides.shape[1]
    row_count = groups * (length // BS)
    positions = jnp.arange(row_count, dtype=jnp.int32)
    onehot = (block_rows[0][None, :] == positions[:, None]).astype(F32)
    high = lax.Precision.HIGHEST

    def everywhere(value):
        return lax.psum(lax.psum(value, ROW), COL)

    def apply_matrix(vector):
        copies = jnp.broadcast_to(vector, (lax.axis_size(ROW), *vector.shape))
        gathered = jnp.moveaxis(swap(copies, ROW), 0, 1).reshape(systems, -1, BS)
        picked = jnp.take(gathered, block_cols[0], axis=1)
        products = jnp.sum(blocks[None] * picked[:, :, None, :], axis=3)
        partial = jnp.einsum("mk,nki->mni", onehot, products, precision=high)
        own = swap(partial.reshape(groups, -1, systems, BS), COL).sum(axis=0)
        return diagonal[None, :] * vector + jnp.transpose(own, (1, 0, 2)).reshape(systems, -1)

    def norm(vector):
        return jnp.sqrt(everywhere(jnp.sum(vector * vector, axis=1)) + epsilon)

    initial_norm = norm(right_sides)
    basis = jnp.zeros((STEPS + 1, systems, length), F32).at[0].set(right_sides / initial_norm[:, None])
    hessenberg = jnp.zeros((systems, STEPS + 1, STEPS), F32)

    def step(j, state):
        basis, hessenberg = state
        candidate = apply_matrix(basis[j])
        coeffs = everywhere(jnp.sum(basis * candidate[None], axis=2).T)
        candidate = candidate - jnp.sum(coeffs.T[:, :, None] * basis, axis=0)
        new_norm = norm(candidate)
        below = (jnp.arange(STEPS + 1) == j + 1).astype(F32)
        column = coeffs + below[None, :] * new_norm[:, None]
        here = (jnp.arange(STEPS) == j).astype(F32)
        hessenberg = hessenberg + column[:, :, None] * here[None, None, :]
        basis = basis.at[j + 1].set(candidate / new_norm[:, None])
        return basis, hessenberg

    basis, hessenberg = lax.fori_loop(0, STEPS, step, (basis, hessenberg))
    weights = least_squares(hessenberg, initial_norm)
    solution = jnp.sum(weights.T[:, :, None] * basis[:STEPS], axis=0)
    return solution, hessenberg


def whole(count):
    return [pl.BlockSpec(memory_space=pltpu.VMEM)] * count


def call(kernel, outs, operands, scratch=(), vmem=24 << 20, name=None):
    return pl.pallas_call(
        kernel,
        out_shape=outs,
        in_specs=whole(len(operands)),
        out_specs=jax.tree.map(lambda o: pl.BlockSpec(memory_space=pltpu.VMEM), outs),
        scratch_shapes=list(scratch),
        compiler_params=pltpu.CompilerParams(vmem_limit_bytes=vmem),
        name=name,
    )(*operands)


def pieces(value, count):
    out = []
    for _ in range(count):
        piece = value.astype(BF16)
        out.append(piece)
        value = value - piece.astype(F32)
    return out


def pick(selector, value, count=3):
    return sum(jnp.dot(selector, piece, preferred_element_type=F32) for piece in pieces(value, count))


PER_CHUNK = 16
AHEAD = 6


def turned_pair(read):
    return jnp.concatenate([read(half).astype(BF16).T for half in range(2)], axis=1)


def gather_sources(got_ref, spread_ref, left_ref):
    sources, slots = got_ref.shape[0], got_ref.shape[1]
    got = got_ref[...].reshape(sources * slots, 2 * BS)
    count = spread_ref.shape[0]
    for at, piece in enumerate(pieces(got, 2)):
        picked = jnp.dot(spread_ref[...], piece, preferred_element_type=F32)
        left_ref[pl.ds(2 * at, count, stride=4), :] = picked[:, :BS]
        left_ref[pl.ds(2 * at + 1, count, stride=4), :] = picked[:, BS:]


def multiply_pair(rows, turned, left_ref, prod_ref):
    upper = lax.broadcasted_iota(jnp.int32, (8, BS), 0) < 4
    both = jnp.dot(left_ref[rows, :].astype(BF16), turned, preferred_element_type=F32)
    prod_ref[rows, :] = jnp.where(upper, both[:, :BS], both[:, BS:])


def sum_targets(prod_ref, sums_ref, out_ref):
    count = sums_ref.shape[1]
    products = jnp.concatenate(
        [prod_ref[pl.ds(n, count, stride=4), :] + prod_ref[pl.ds(n + 2, count, stride=4), :] for n in range(2)],
        axis=1,
    )
    out_ref[...] = pick(sums_ref[...], products).reshape(out_ref.shape)


def first_product_kernel(
    got_ref, spread_ref, blocks_ref, sums_ref, lists_ref, out_ref, turned_ref, left_ref, prod_ref, held_ref, sem
):
    chunks, per_chunk = held_ref.shape[0], held_ref.shape[1]
    pairs = per_chunk // 2

    def fetch(chunk):
        start = pl.multiple_of(chunk * per_chunk, per_chunk)
        return pltpu.make_async_copy(blocks_ref.at[pl.ds(start, per_chunk)], held_ref.at[chunk], sem.at[chunk])

    for chunk in range(AHEAD):
        fetch(chunk).start()
    gather_sources(got_ref, spread_ref, left_ref)

    def one(chunk, carry):
        fetch(chunk).wait()

        @pl.when(chunk + AHEAD < chunks)
        def _():
            fetch(chunk + AHEAD).start()

        for pair in range(pairs):
            turned = turned_pair(lambda half: held_ref[chunk, 2 * pair + half])
            at = chunk * pairs + pair
            turned_ref[at] = turned
            multiply_pair(pl.ds(pl.multiple_of(8 * at, 8), 8), turned, left_ref, prod_ref)
        return carry

    lax.fori_loop(0, chunks, one, 0)
    sum_targets(prod_ref, sums_ref, out_ref)
    targets, slots = out_ref.shape[0], out_ref.shape[1]
    for t in range(targets):
        out_ref[t, slots - 1 : slots, :] = lists_ref[...].astype(F32) - float(t * BS)


def product_kernel(got_ref, spread_ref, turned_ref, sums_ref, out_ref, left_ref, prod_ref):
    gather_sources(got_ref, spread_ref, left_ref)
    for pair in range(turned_ref.shape[0]):
        multiply_pair(slice(8 * pair, 8 * pair + 8), turned_ref[pair], left_ref, prod_ref)
    sum_targets(prod_ref, sums_ref, out_ref)
    slots = out_ref.shape[1]
    ride = ridden(got_ref)
    for t in range(out_ref.shape[0]):
        out_ref[t, slots - 1 : slots, :] = ride


def first_products(got, spread, blocks, sums, lists):
    count = spread.shape[0]
    targets = sums.shape[0] // DST_SLOTS
    chunks = count // PER_CHUNK
    specs = whole(5)
    specs[2] = pl.BlockSpec(memory_space=pltpu.HBM)
    return pl.pallas_call(
        first_product_kernel,
        out_shape=(
            jax.ShapeDtypeStruct((targets, DST_SLOTS, 2 * BS), F32),
            jax.ShapeDtypeStruct((count // 2, BS, 2 * BS), BF16),
        ),
        in_specs=specs,
        out_specs=(pl.BlockSpec(memory_space=pltpu.VMEM), pl.BlockSpec(memory_space=pltpu.VMEM)),
        scratch_shapes=[
            pltpu.VMEM((4 * count, BS), F32),
            pltpu.VMEM((4 * count, BS), F32),
            pltpu.VMEM((chunks, PER_CHUNK, BS, BS), F32),
            pltpu.SemaphoreType.DMA((chunks,)),
        ],
        compiler_params=pltpu.CompilerParams(vmem_limit_bytes=32 << 20),
        name="first_products",
    )(got, spread, blocks, sums, lists)


def block_products(got, spread, turned, sums):
    count = spread.shape[0]
    targets = sums.shape[0] // DST_SLOTS
    return call(
        product_kernel,
        jax.ShapeDtypeStruct((targets, DST_SLOTS, 2 * BS), F32),
        (got, spread, turned, sums),
        [pltpu.VMEM((4 * count, BS), F32), pltpu.VMEM((4 * count, BS), F32)],
        vmem=16 << 20,
        name="block_products",
    )


def lane_of(row, lane):
    return row[:, lane : lane + 1]


def total(value):
    return jnp.sum(value, axis=0, keepdims=True)


def send_out(values, wanted_ref, ride, out_ref):
    out = pick(wanted_ref[...], values)
    out_ref[...] = out.reshape(out_ref.shape)
    slots = out_ref.shape[1]
    for s in range(out_ref.shape[0]):
        out_ref[s, slots - 1 : slots, :] = ride


def ranks(present):
    shape = (BS, BS)
    before = lax.broadcasted_iota(jnp.int32, shape, 0) < lax.broadcasted_iota(jnp.int32, shape, 1)
    return jnp.dot(present.astype(BF16), before.astype(F32).astype(BF16), preferred_element_type=F32)


def present_in(column, offset):
    lane = lax.broadcasted_iota(jnp.int32, (column.shape[0], BS), 1).astype(F32) + offset
    return jnp.max(jnp.where(column == lane, 1.0, 0.0), axis=0, keepdims=True)


def slot_rows(present, rank, slots, usable):
    at = lax.broadcasted_iota(jnp.int32, (slots, BS), 0).astype(F32)
    return jnp.where((rank == at) & (present > 0.0) & (at < usable), 1.0, 0.0)


def one_hots(lists, slots):
    columns = lists.T
    present = jnp.concatenate([present_in(columns[:, g : g + 1], 0.0) for g in range(lists.shape[0])], axis=0)
    rank = ranks(present)
    return jnp.concatenate(
        [slot_rows(present[g : g + 1], rank[g : g + 1], slots, slots - 1.0) for g in range(lists.shape[0])], axis=0
    )


def slot_column(index, groups, slots):
    column = jnp.broadcast_to(index, (8, index.shape[1])).T[:, :1]
    present = jnp.concatenate([present_in(column, float(g * BS)) for g in range(groups)], axis=0)
    rank = ranks(present)
    lane = lax.broadcasted_iota(jnp.int32, (column.shape[0], BS), 1).astype(F32)
    found = jnp.zeros(lane.shape, F32)
    for g in range(groups):
        found = found + jnp.where(column == lane + float(g * BS), rank[g : g + 1] + float(g * slots), 0.0)
    largest = jnp.max(jnp.sum(present, axis=1, keepdims=True), axis=0, keepdims=True)
    return jnp.sum(found, axis=1, keepdims=True), largest


def plan_kernel(sources, targets, cols_ref, rows_ref, spread_ref, sums_ref, over_ref):
    count = cols_ref.shape[1]
    column, src_most = slot_column(cols_ref[...].astype(F32), sources, SRC_SLOTS)
    at = lax.broadcasted_iota(jnp.int32, spread_ref.shape, 1).astype(F32)
    spread_ref[...] = jnp.where(column == at, 1.0, 0.0).astype(BF16)
    column, dst_most = slot_column(rows_ref[...].astype(F32), targets, DST_SLOTS)
    row = jnp.broadcast_to(column, (count, BS)).T[:1, :]
    at = lax.broadcasted_iota(jnp.int32, sums_ref.shape, 0).astype(F32)
    sums_ref[...] = jnp.where(row == at, 1.0, 0.0).astype(BF16)
    over = jnp.where((src_most > SRC_SLOTS - 1.0) | (dst_most > DST_SLOTS - 1.0), 1.0, 0.0)
    lane = lax.broadcasted_iota(jnp.int32, over_ref.shape, 1)
    over_ref[...] = jnp.where(lane == BS + FLAG, over, 0.0)


def start_kernel(asked_ref, b_ref, wanted_ref, out_ref):
    lists = jnp.concatenate([asked_ref[g, 0:1, :] for g in range(asked_ref.shape[0])], axis=0)
    wanted_ref[...] = one_hots(lists, SRC_SLOTS).astype(BF16)
    send_out(side_by_side(b_ref), wanted_ref, jnp.zeros((1, 2 * BS), F32), out_ref)


def inner_products(dots_ref, vs, q, p, j):
    rides = []
    for n in range(2):
        cut = slice(n * BS, (n + 1) * BS)
        dots_ref[...] = jnp.zeros(dots_ref.shape, F32)
        qn, pn = q[:, cut], p[:, cut]
        for i in range(j):
            vn = vs[i][:, cut]
            dots_ref[i : i + 1, :] = total(vn * pn)
            dots_ref[GRAM + i : GRAM + i + 1, :] = total(vn * qn)
        dots_ref[j : j + 1, :] = total(qn * pn)
        dots_ref[QQ : QQ + 1, :] = total(qn * qn)
        dots_ref[PP : PP + 1, :] = total(pn * pn)
        ones = jnp.ones((8, BS), F32)
        row = lax.dot_general(
            ones, dots_ref[...], (((1,), (1,)), ((), ())),
            precision=lax.Precision.HIGHEST, preferred_element_type=F32,
        )
        rides.append(row[0:1, :])
    return jnp.concatenate(rides, axis=1)


def arrived(got_ref, scatter_ref):
    flat = got_ref[...].reshape(-1, 2 * BS)
    return pick(scatter_ref[...], flat)


def ridden(got_ref):
    slots = got_ref.shape[1]
    ride = got_ref[0, slots - 1 : slots, :]
    for s in range(1, got_ref.shape[0]):
        ride = ride + got_ref[s, slots - 1 : slots, :]
    return ride


def side_by_side(ref):
    return jnp.concatenate([ref[0], ref[1]], axis=1)


def first_kernel(got_ref, over_ref, b_ref, diag_ref, wanted_ref, scatter_ref, p_ref, q_ref, out_ref, dots_ref):
    slots = got_ref.shape[1]
    lists = jnp.concatenate([got_ref[g, slots - 1 : slots, :] for g in range(got_ref.shape[0])], axis=0)
    scatter_ref[...] = one_hots(lists, DST_SLOTS).T.astype(BF16)
    b = side_by_side(b_ref)
    p = arrived(got_ref, scatter_ref) + jnp.concatenate([diag_ref[...]] * 2, axis=1) * b
    p_ref[...] = p
    q_ref[...] = b
    send_out(p, wanted_ref, inner_products(dots_ref, [], b, p, 0) + over_ref[0:1, :], out_ref)


def column_of(ride, j):
    lane = lax.broadcasted_iota(jnp.int32, (1, BS), 1)
    out = []
    for n in range(2):
        row = ride[:, n * BS : (n + 1) * BS]
        inverse = 1.0 / jnp.sqrt(lane_of(row, QQ) + epsilon)
        h = row * jnp.where(lane == j, inverse * inverse, jnp.broadcast_to(inverse, (1, BS)))
        out.append((h, inverse))
    return out


def step_kernel(j, *refs):
    got_ref, scatter_ref, q_ref, p_ref, diag_ref, wanted_ref = refs[:6]
    v_refs = refs[6 : 6 + j]
    m_refs = refs[6 + j : 6 + 2 * j]
    v_ref, m_ref, q_out, p_out, ride_out, out_ref, dots_ref = refs[6 + 2 * j :]
    ride = ridden(got_ref)
    ride_out[...] = jnp.broadcast_to(ride, ride_out.shape)
    coeffs = column_of(ride, j)
    z = arrived(got_ref, scatter_ref)
    for n, (h, inverse) in enumerate(coeffs):
        cut = slice(n * BS, (n + 1) * BS)
        pn = p_ref[:, cut]
        v = q_ref[:, cut] * inverse
        m = pn * inverse
        v_ref[:, cut] = v
        m_ref[:, cut] = m
        q_next = m - lane_of(h, j) * v
        p_next = (z[:, cut] + diag_ref[...] * pn) * inverse - lane_of(h, j) * m
        for i in range(j):
            q_next = q_next - lane_of(h, i) * v_refs[i][:, cut]
            p_next = p_next - lane_of(h, i) * m_refs[i][:, cut]
        q_out[:, cut] = q_next
        p_out[:, cut] = p_next
    p = p_out[...]
    ride = inner_products(dots_ref, [r[...] for r in v_refs] + [v_ref[...]], q_out[...], p, j + 1)
    if j + 1 == STEPS - 1:
        out_ref[...] = jnp.broadcast_to(ride[:, None, :], out_ref.shape)
    else:
        send_out(p, wanted_ref, ride, out_ref)


GRAM_AT, NUMBERS_AT = 16, 24
KEPT_ROWS = 96


def rotations_kernel(*refs):
    ride_refs, kept_ref = refs[:-1], refs[-1]
    rides = [r[0:1, :] for r in ride_refs]
    per_step = [column_of(ride, j) for j, ride in enumerate(rides)]
    lane = lax.broadcasted_iota(jnp.int32, (1, BS), 1)
    known = len(rides)
    kept_ref[...] = jnp.zeros(kept_ref.shape, F32)
    for n in range(2):
        rows = [ride[:, n * BS : (n + 1) * BS] for ride in rides]
        norms = [jnp.sqrt(lane_of(row, QQ) + epsilon) for row in rows]
        inverses = [per_step[j][n][1] for j in range(known)]
        for j in range(known):
            column = jnp.where(lane <= j, per_step[j][n][0], 0.0)
            if j + 1 < known:
                column = jnp.where(lane == j + 1, norms[j + 1], column)
            kept_ref[n, j : j + 1, :] = column
            gram = pltpu.roll(rows[j], BS - GRAM, 1) * inverses[j]
            own = lane_of(rows[j], QQ) * inverses[j] * inverses[j]
            gram = jnp.where(lane < j, 2.0 * gram, 0.0)
            kept_ref[n, GRAM_AT + j : GRAM_AT + j + 1, :] = jnp.where(lane == j, own, gram)
        targets = [norms[0]] + [jnp.zeros_like(norms[0])] * known
        cosines, sines, triangle = [], [], []
        for j in range(known - 1):
            column = [lane_of(per_step[j][n][0], i) for i in range(j + 1)]
            rotate(column + [norms[j + 1]], cosines, sines, targets, triangle)
        numbers = cosines + sines + [x for column in triangle for x in column] + targets[:known]
        for at, number in enumerate(numbers):
            kept_ref[n, NUMBERS_AT + at : NUMBERS_AT + at + 1, :] = jnp.broadcast_to(number, (1, BS))


def finish_kernel(last_ref, kept_ref, q_ref, *refs):
    v_refs, (solution_ref, hessenberg_ref) = refs[:-2], refs[-2:]
    known = STEPS - 1
    ride = jnp.sum(last_ref[...], axis=0)
    lane = lax.broadcasted_iota(jnp.int32, (1, BS), 1)
    both = []
    for n, (h, inverse) in enumerate(column_of(ride, known)):
        row = ride[:, n * BS : (n + 1) * BS]
        norm = jnp.sqrt(lane_of(row, QQ) + epsilon)
        h = jnp.where(lane <= known, h, 0.0)
        gram = jnp.where(lane < known, 2.0 * pltpu.roll(row, BS - GRAM, 1) * inverse, 0.0)
        gram = jnp.where(lane == known, lane_of(row, QQ) * inverse * inverse, gram)
        table = jnp.concatenate([kept_ref[n, GRAM_AT : GRAM_AT + known, :], gram], axis=0)
        column = jnp.broadcast_to(h, (8, BS)).T[:8, :1]
        form = jnp.sum(jnp.sum(table * h * column, axis=1, keepdims=True), axis=0, keepdims=True)
        twice = 2.0 * jnp.sum(h * h, axis=1, keepdims=True)
        remainder = lane_of(row, PP) * inverse * inverse - twice + form
        final_norm = jnp.sqrt(jnp.maximum(remainder, 0.0) + epsilon)
        columns = jnp.concatenate([kept_ref[n, :known, :], jnp.where(lane == known + 1, final_norm, h)], axis=0)
        before_last = lax.broadcasted_iota(jnp.int32, columns.shape, 0) == known - 1
        columns = jnp.where(before_last & (lane == known), norm, columns)
        hessenberg_ref[n] = columns.T[: STEPS + 1, :]

        def number(at):
            return kept_ref[n, NUMBERS_AT + at : NUMBERS_AT + at + 1, :]

        cosines = [number(i) for i in range(known - 1)]
        sines = [number(known - 1 + i) for i in range(known - 1)]
        at, triangle = 2 * (known - 1), []
        for j in range(known - 1):
            triangle.append([number(at + i) for i in range(j + 1)])
            at += j + 1
        targets = [number(at + i) for i in range(known)] + [None, None]
        wide = jnp.zeros((1, BS), F32)
        previous = kept_ref[n, known - 1 : known, :]
        column = [wide + lane_of(previous, i) for i in range(known)] + [wide + norm]
        rotate(column, cosines, sines, targets, triangle)
        column = [wide + lane_of(h, i) for i in range(STEPS)] + [wide + final_norm]
        rotate(column, cosines, sines, targets, triangle)
        weights = back_substitute(triangle, targets)
        cut = slice(n * BS, (n + 1) * BS)
        acc = (weights[-1] * inverse) * q_ref[:, cut]
        for i in range(STEPS - 1):
            acc = acc + weights[i] * v_refs[i][:, cut]
        both.append(acc)
    for block in range(BS):
        row = jnp.concatenate([acc[block : block + 1, :] for acc in both], axis=0)
        solution_ref[:, block * BS : (block + 1) * BS] = row


def body(blocks, block_rows, block_cols, diagonal, right_sides):
    rows_n, cols_n = lax.axis_size(ROW), lax.axis_size(COL)
    count = blocks.shape[0]
    b = right_sides.reshape(2, -1, BS)
    diag = diagonal.reshape(-1, BS)

    group = jnp.arange(rows_n, dtype=jnp.int32)[:, None, None]
    relative = (block_cols[None] - group * BS).astype(F32)
    asked = swap(jnp.broadcast_to(relative, (rows_n, 8, count)), ROW)
    spread, sums, over = call(
        functools.partial(plan_kernel, rows_n, cols_n),
        (
            jax.ShapeDtypeStruct((count, rows_n * SRC_SLOTS), BF16),
            jax.ShapeDtypeStruct((cols_n * DST_SLOTS, count), BF16),
            jax.ShapeDtypeStruct((8, 2 * BS), F32),
        ),
        (block_cols, block_rows),
        name="plan",
    )

    out_shape = jax.ShapeDtypeStruct((rows_n, SRC_SLOTS, 2 * BS), F32)
    vec = jax.ShapeDtypeStruct((BS, 2 * BS), F32)
    dots = pltpu.VMEM((BS, BS), F32)

    wanted, send = call(
        start_kernel, (jax.ShapeDtypeStruct((rows_n * SRC_SLOTS, BS), BF16), out_shape), (asked, b), name="start"
    )
    partial, turned = first_products(swap(send, ROW), spread, blocks, sums, block_rows)
    got = swap(partial, COL)
    scatter, p, q, send = call(
        first_kernel,
        (jax.ShapeDtypeStruct((BS, cols_n * DST_SLOTS), BF16), vec, vec, out_shape),
        (got, over, b, diag, wanted),
        [dots],
        name="first",
    )
    vs, ms, rides = [], [], []
    for j in range(STEPS - 1):
        got = swap(block_products(swap(send, ROW), spread, turned, sums), COL)
        last = j + 1 == STEPS - 1
        outs = (
            vec, vec, vec, vec, jax.ShapeDtypeStruct((8, 2 * BS), F32),
            jax.ShapeDtypeStruct((rows_n * cols_n, 1, 2 * BS), F32) if last else out_shape,
        )
        v, m, q, p, ride, send = call(
            functools.partial(step_kernel, j), outs, (got, scatter, q, p, diag, wanted, *vs, *ms), [dots],
            name=f"step_{j}",
        )
        vs.append(v)
        ms.append(m)
        rides.append(ride)
    final = swap(send, BOTH)
    so_far = call(
        rotations_kernel, jax.ShapeDtypeStruct((2, KEPT_ROWS, BS), F32), tuple(rides), name="rotations"
    )

    def compact(final, so_far, q, *vs):
        solution, hessenberg = call(
            finish_kernel,
            (
                jax.ShapeDtypeStruct((2, BS * BS), F32),
                jax.ShapeDtypeStruct((2, STEPS + 1, STEPS), F32),
            ),
            (final, so_far, q, *vs),
            name="finish",
        )
        return solution, hessenberg

    return lax.cond(
        rides[0][0, BS + FLAG] > 0.0,
        lambda *args: dense_cycle(*args[:5]),
        lambda *args: compact(*args[5:]),
        blocks, block_rows, block_cols, diagonal, right_sides, final, so_far, q, *vs,
    )


def solution(mesh):
    placed = (P(BOTH, None, None), P(BOTH, None), P(BOTH, None), P(BOTH), P(None, BOTH))
    return jax.shard_map(
        body, mesh=mesh, in_specs=placed, out_specs=(P(None, BOTH), P()), check_vma=False
    )
```

```python
import functools

import jax
import jax.numpy as jnp
from jax import lax
from jax.experimental import pallas as pl
from jax.experimental.pallas import tpu as pltpu
from jax.sharding import PartitionSpec as P

STEPS = 8
BS = 128
SRC_SLOTS = 56
DST_SLOTS = 24
ROW = "row"
COL = "col"
BOTH = ("row", "col")
F32 = jnp.float32
BF16 = jnp.bfloat16

epsilon = 1e-06

QQ, PP, GRAM, FLAG = 9, 10, 16, 127


def swap(value, axis):
    return lax.all_to_all(value, axis, split_axis=0, concat_axis=0, tiled=True)


def least_squares(hessenberg, initial_norm):
    total_steps = hessenberg.shape[2]
    targets = [initial_norm] + [jnp.zeros_like(initial_norm) for j in range(total_steps)]
    cosines, sines, triangle = ([], [], [])
    for j in range(total_steps):
        column = [hessenberg[:, i, j] for i in range(j + 2)]
        rotate(column, cosines, sines, targets, triangle)
    return jnp.stack(back_substitute(triangle, targets), axis=1)


def rotate(column, cosines, sines, targets, triangle):
    j = len(column) - 2
    for i in range(j):
        leading, trailing = (column[i], column[i + 1])
        column[i] = cosines[i] * leading + sines[i] * trailing
        column[i + 1] = cosines[i] * trailing - sines[i] * leading
    radius = jnp.sqrt(column[j] * column[j] + column[j + 1] * column[j + 1])
    cosine = column[j] / radius
    sine_term = column[j + 1] / radius
    column[j] = radius
    cosines.append(cosine)
    sines.append(sine_term)
    targets[j + 1] = -sine_term * targets[j]
    targets[j] = cosine * targets[j]
    triangle.append(column[: j + 1])


def back_substitute(triangle, targets):
    total_steps = len(triangle)
    coeffs = [None] * total_steps
    for j in reversed(range(total_steps)):
        running = targets[j]
        for k in range(j + 1, total_steps):
            running = running - triangle[k][j] * coeffs[k]
        coeffs[j] = running / triangle[j][j]
    return coeffs


def dense_cycle(blocks, block_rows, block_cols, diagonal, right_sides):
    systems = right_sides.shape[0]
    groups = lax.axis_size(COL)
    length = right_sides.shape[1]
    row_count = groups * (length // BS)
    positions = jnp.arange(row_count, dtype=jnp.int32)
    onehot = (block_rows[0][None, :] == positions[:, None]).astype(F32)
    high = lax.Precision.HIGHEST

    def everywhere(value):
        return lax.psum(lax.psum(value, ROW), COL)

    def apply_matrix(vector):
        copies = jnp.broadcast_to(vector, (lax.axis_size(ROW), *vector.shape))
        gathered = jnp.moveaxis(swap(copies, ROW), 0, 1).reshape(systems, -1, BS)
        picked = jnp.take(gathered, block_cols[0], axis=1)
        products = jnp.sum(blocks[None] * picked[:, :, None, :], axis=3)
        partial = jnp.einsum("mk,nki->mni", onehot, products, precision=high)
        own = swap(partial.reshape(groups, -1, systems, BS), COL).sum(axis=0)
        return diagonal[None, :] * vector + jnp.transpose(own, (1, 0, 2)).reshape(systems, -1)

    def norm(vector):
        return jnp.sqrt(everywhere(jnp.sum(vector * vector, axis=1)) + epsilon)

    initial_norm = norm(right_sides)
    basis = jnp.zeros((STEPS + 1, systems, length), F32).at[0].set(right_sides / initial_norm[:, None])
    hessenberg = jnp.zeros((systems, STEPS + 1, STEPS), F32)

    def step(j, state):
        basis, hessenberg = state
        candidate = apply_matrix(basis[j])
        coeffs = everywhere(jnp.sum(basis * candidate[None], axis=2).T)
        candidate = candidate - jnp.sum(coeffs.T[:, :, None] * basis, axis=0)
        new_norm = norm(candidate)
        below = (jnp.arange(STEPS + 1) == j + 1).astype(F32)
        column = coeffs + below[None, :] * new_norm[:, None]
        here = (jnp.arange(STEPS) == j).astype(F32)
        hessenberg = hessenberg + column[:, :, None] * here[None, None, :]
        basis = basis.at[j + 1].set(candidate / new_norm[:, None])
        return basis, hessenberg

    basis, hessenberg = lax.fori_loop(0, STEPS, step, (basis, hessenberg))
    weights = least_squares(hessenberg, initial_norm)
    solution = jnp.sum(weights.T[:, :, None] * basis[:STEPS], axis=0)
    return solution, hessenberg


def whole(count):
    return [pl.BlockSpec(memory_space=pltpu.VMEM)] * count


def call(kernel, outs, operands, scratch=(), vmem=24 << 20, name=None):
    return pl.pallas_call(
        kernel,
        out_shape=outs,
        in_specs=whole(len(operands)),
        out_specs=jax.tree.map(lambda o: pl.BlockSpec(memory_space=pltpu.VMEM), outs),
        scratch_shapes=list(scratch),
        compiler_params=pltpu.CompilerParams(vmem_limit_bytes=vmem),
        name=name,
    )(*operands)


def pieces(value, count):
    out = []
    for _ in range(count):
        piece = value.astype(BF16)
        out.append(piece)
        value = value - piece.astype(F32)
    return out


def pick(selector, value, count=3):
    return sum(jnp.dot(selector, piece, preferred_element_type=F32) for piece in pieces(value, count))


CHUNKS = 8


def turn_kernel(blocks_ref, turned_ref, held_ref, made_ref, arrived_sem, left_sem):
    steps, per_step = held_ref.shape[0], held_ref.shape[1]
    pairs = per_step // 2

    def fetch(step):
        return pltpu.make_async_copy(
            blocks_ref.at[pl.ds(pl.multiple_of(step * per_step, per_step), per_step)],
            held_ref.at[step],
            arrived_sem.at[step],
        )

    def keep(step):
        return pltpu.make_async_copy(
            made_ref.at[step],
            turned_ref.at[pl.ds(pl.multiple_of(step * pairs, pairs), pairs)],
            left_sem.at[step],
        )

    for step in range(steps):
        fetch(step).start()

    def one(step, carry):
        fetch(step).wait()
        for pair in range(pairs):
            made_ref[step, pair] = jnp.concatenate(
                [held_ref[step, 2 * pair + half].astype(BF16).T for half in range(2)], axis=1
            )
        keep(step).start()
        return carry

    lax.fori_loop(0, steps, one, 0)
    for step in range(steps):
        keep(step).wait()


def turn_blocks(blocks, per_step=16):
    count = blocks.shape[0]
    steps = count // per_step
    return pl.pallas_call(
        turn_kernel,
        out_shape=pltpu.MemorySpace.HBM((count // 2, BS, 2 * BS), BF16),
        in_specs=[pl.BlockSpec(memory_space=pltpu.HBM)],
        out_specs=pl.BlockSpec(memory_space=pltpu.HBM),
        scratch_shapes=[
            pltpu.VMEM((steps, per_step, BS, BS), F32),
            pltpu.VMEM((steps, per_step // 2, BS, 2 * BS), BF16),
            pltpu.SemaphoreType.DMA((steps,)),
            pltpu.SemaphoreType.DMA((steps,)),
        ],
        compiler_params=pltpu.CompilerParams(vmem_limit_bytes=28 << 20),
        cost_estimate=pl.CostEstimate(flops=40_000_000, transcendentals=0, bytes_accessed=count * BS * BS * 6),
        name="turn_blocks",
    )(blocks)


def gather_sources(got_ref, spread_ref, left_ref):
    sources, slots = got_ref.shape[0], got_ref.shape[1]
    got = got_ref[...].reshape(sources * slots, 2 * BS)
    count = spread_ref.shape[0]
    for at, piece in enumerate(pieces(got, 2)):
        picked = jnp.dot(spread_ref[...], piece, preferred_element_type=F32)
        left_ref[pl.ds(2 * at, count, stride=4), :] = picked[:, :BS]
        left_ref[pl.ds(2 * at + 1, count, stride=4), :] = picked[:, BS:]


def multiply_pair(rows, turned, left_ref, prod_ref):
    upper = lax.broadcasted_iota(jnp.int32, (8, BS), 0) < 4
    both = jnp.dot(left_ref[rows, :].astype(BF16), turned, preferred_element_type=F32)
    prod_ref[rows, :] = jnp.where(upper, both[:, :BS], both[:, BS:])


def sum_targets(prod_ref, sums_ref, out_ref):
    count = sums_ref.shape[1]
    products = jnp.concatenate(
        [prod_ref[pl.ds(n, count, stride=4), :] + prod_ref[pl.ds(n + 2, count, stride=4), :] for n in range(2)],
        axis=1,
    )
    out_ref[...] = pick(sums_ref[...], products).reshape(out_ref.shape)


def first_product_kernel(
    got_ref, spread_ref, stored_ref, sums_ref, lists_ref, out_ref, turned_ref, wanted_ref, left_ref, prod_ref, sem
):
    per_chunk = stored_ref.shape[0] // CHUNKS

    def fetch(chunk):
        where = pl.ds(pl.multiple_of(chunk * per_chunk, per_chunk), per_chunk)
        return pltpu.make_async_copy(stored_ref.at[where], turned_ref.at[where], sem.at[chunk])

    for chunk in range(CHUNKS):
        fetch(chunk).start()
    gather_sources(got_ref, spread_ref, left_ref)
    asked = jnp.concatenate([got_ref[g, BS : BS + 1, :] for g in range(got_ref.shape[0])], axis=0)
    wanted_ref[...] = one_hots(asked, SRC_SLOTS).astype(BF16)

    def one(chunk, carry):
        fetch(chunk).wait()
        for k in range(per_chunk):
            pair = chunk * per_chunk + k
            multiply_pair(pl.ds(pl.multiple_of(8 * pair, 8), 8), turned_ref[pair], left_ref, prod_ref)
        return carry

    lax.fori_loop(0, CHUNKS, one, 0)
    sum_targets(prod_ref, sums_ref, out_ref)
    targets, slots = out_ref.shape[0], out_ref.shape[1]
    lists = lists_ref[0:1, :]
    for t in range(targets):
        own = pltpu.roll(lists, lists.shape[1] - t * slots, 1) if t else lists
        out_ref[t, slots - 1 : slots, :] = own[:, : 2 * BS]


def product_kernel(got_ref, spread_ref, turned_ref, sums_ref, out_ref, left_ref, prod_ref):
    gather_sources(got_ref, spread_ref, left_ref)

    def one(pair, carry):
        multiply_pair(pl.ds(pl.multiple_of(8 * pair, 8), 8), turned_ref[pair], left_ref, prod_ref)
        return carry

    lax.fori_loop(0, turned_ref.shape[0], one, 0, unroll=64)
    sum_targets(prod_ref, sums_ref, out_ref)
    slots = out_ref.shape[1]
    ride = ridden(got_ref)
    for t in range(out_ref.shape[0]):
        out_ref[t, slots - 1 : slots, :] = ride


def first_products(got, spread, stored, sums, lists):
    count = spread.shape[0]
    sources = got.shape[0]
    targets = sums.shape[0] // DST_SLOTS
    specs = whole(5)
    specs[2] = pl.BlockSpec(memory_space=pltpu.HBM)
    outs = (
        jax.ShapeDtypeStruct((targets, DST_SLOTS, 2 * BS), F32),
        jax.ShapeDtypeStruct(stored.shape, BF16),
        jax.ShapeDtypeStruct((sources * SRC_SLOTS, BS), BF16),
    )
    return pl.pallas_call(
        first_product_kernel,
        out_shape=outs,
        in_specs=specs,
        out_specs=tuple(whole(3)),
        scratch_shapes=[
            pltpu.VMEM((4 * count, BS), F32),
            pltpu.VMEM((4 * count, BS), F32),
            pltpu.SemaphoreType.DMA((CHUNKS,)),
        ],
        compiler_params=pltpu.CompilerParams(vmem_limit_bytes=24 << 20),
        name="first_products",
    )(got, spread, pltpu.with_memory_space_constraint(stored, pltpu.HBM), sums, lists)


def block_products(got, spread, turned, sums):
    count = spread.shape[0]
    targets = sums.shape[0] // DST_SLOTS
    return call(
        product_kernel,
        jax.ShapeDtypeStruct((targets, DST_SLOTS, 2 * BS), F32),
        (got, spread, turned, sums),
        [pltpu.VMEM((4 * count, BS), F32), pltpu.VMEM((4 * count, BS), F32)],
        vmem=16 << 20,
        name="block_products",
    )


def lane_of(row, lane):
    return row[:, lane : lane + 1]


def total(value):
    return jnp.sum(value, axis=0, keepdims=True)


def send_out(values, wanted_ref, ride, out_ref):
    out = pick(wanted_ref[...], values)
    out_ref[...] = out.reshape(out_ref.shape)
    slots = out_ref.shape[1]
    for s in range(out_ref.shape[0]):
        out_ref[s, slots - 1 : slots, :] = ride


def ranks(present):
    shape = (BS, BS)
    before = lax.broadcasted_iota(jnp.int32, shape, 0) < lax.broadcasted_iota(jnp.int32, shape, 1)
    return jnp.dot(present.astype(BF16), before.astype(F32).astype(BF16), preferred_element_type=F32)


def present_in(column, offset):
    lane = lax.broadcasted_iota(jnp.int32, (column.shape[0], BS), 1).astype(F32) + offset
    return jnp.max(jnp.where(column == lane, 1.0, 0.0), axis=0, keepdims=True)


def slot_rows(present, rank, slots, usable):
    at = lax.broadcasted_iota(jnp.int32, (slots, BS), 0).astype(F32)
    return jnp.where((rank == at) & (present > 0.0) & (at < usable), 1.0, 0.0)


def one_hots(lists, slots):
    columns = lists.T
    present = jnp.concatenate([present_in(columns[:, g : g + 1], 0.0) for g in range(lists.shape[0])], axis=0)
    rank = ranks(present)
    return jnp.concatenate(
        [slot_rows(present[g : g + 1], rank[g : g + 1], slots, slots - 1.0) for g in range(lists.shape[0])], axis=0
    )


def plan_kernel(sources, targets, cols_ref, rows_ref, whole_ref, spread_ref, sums_ref, lists_ref, over_ref):
    count = cols_ref.shape[1]

    def column_of_blocks(ref):
        return jnp.broadcast_to(ref[...].astype(F32), (8, count)).T[:, :1]

    def present_and_rank(column, groups):
        present = jnp.concatenate([present_in(column, float(g * BS)) for g in range(groups)], axis=0)
        return present, ranks(present)

    def slot_column(column, rank, groups, slots):
        lane = lax.broadcasted_iota(jnp.int32, (count, BS), 1).astype(F32)
        found = jnp.zeros(lane.shape, F32)
        for g in range(groups):
            found = found + jnp.where(column == lane + float(g * BS), rank[g : g + 1] + float(g * slots), 0.0)
        return jnp.sum(found, axis=1, keepdims=True)

    def most(present):
        return jnp.max(jnp.sum(present, axis=1, keepdims=True), axis=0, keepdims=True)

    column = column_of_blocks(cols_ref)
    present, rank = present_and_rank(column, sources)
    slot = slot_column(column, rank, sources, SRC_SLOTS)
    at = lax.broadcasted_iota(jnp.int32, spread_ref.shape, 1).astype(F32)
    spread_ref[...] = jnp.where(slot == at, 1.0, 0.0).astype(BF16)
    pitch = whole_ref.shape[1] // sources
    at = lax.broadcasted_iota(jnp.int32, (count, pitch), 1).astype(F32)
    in_group = jnp.concatenate(
        [jnp.where((column - float(g * BS) == at) & (at < BS), 1.0, 0.0) for g in range(sources)], axis=1
    )
    whole_ref[...] = in_group.astype(BF16)
    over = most(present) > SRC_SLOTS - 1.0

    column = column_of_blocks(rows_ref)
    present, rank = present_and_rank(column, targets)
    slot = slot_column(column, rank, targets, DST_SLOTS)
    row = jnp.broadcast_to(slot, (count, BS)).T[:1, :]
    at = lax.broadcasted_iota(jnp.int32, sums_ref.shape, 0).astype(F32)
    sums_ref[...] = jnp.where(row == at, 1.0, 0.0).astype(BF16)
    listed = jnp.concatenate(
        [slot_rows(present[t : t + 1], rank[t : t + 1], DST_SLOTS, DST_SLOTS - 1.0) for t in range(targets)], axis=0
    )
    number = lax.broadcasted_iota(jnp.int32, (8, BS), 1).astype(F32) + 1.0
    lists_ref[...] = lax.dot_general(
        number.astype(BF16), listed.astype(BF16), (((1,), (1,)), ((), ())), preferred_element_type=F32
    ) - 1.0
    over = jnp.where(over | (most(present) > DST_SLOTS - 1.0), 1.0, 0.0)
    lane = lax.broadcasted_iota(jnp.int32, over_ref.shape, 1)
    over_ref[...] = jnp.where(lane == BS + FLAG, over, 0.0)


def open_kernel(sides_ref, cols_ref, out_ref, b_ref):
    for at in range(0, BS, 8):
        tiles = [sides_ref[:, (at + k) * BS : (at + k + 1) * BS] for k in range(8)]
        for n in range(2):
            b_ref[at : at + 8, n * BS : (n + 1) * BS] = jnp.concatenate([t[n : n + 1, :] for t in tiles], axis=0)
    below = lax.broadcasted_iota(jnp.int32, (8, 2 * BS), 0) == 0
    cols = cols_ref[...].astype(F32)
    for g in range(out_ref.shape[0]):
        out_ref[g, :BS, :] = b_ref[...]
        out_ref[g, BS:, :] = jnp.where(below, cols - float(g * BS), 0.0)


def inner_products(dots_ref, vs, q, p, j):
    rides = []
    for n in range(2):
        cut = slice(n * BS, (n + 1) * BS)
        dots_ref[...] = jnp.zeros(dots_ref.shape, F32)
        qn, pn = q[:, cut], p[:, cut]
        for i in range(j):
            vn = vs[i][:, cut]
            dots_ref[i : i + 1, :] = total(vn * pn)
            dots_ref[GRAM + i : GRAM + i + 1, :] = total(vn * qn)
        dots_ref[j : j + 1, :] = total(qn * pn)
        dots_ref[QQ : QQ + 1, :] = total(qn * qn)
        dots_ref[PP : PP + 1, :] = total(pn * pn)
        ones = jnp.ones((8, BS), F32)
        row = lax.dot_general(
            ones, dots_ref[...], (((1,), (1,)), ((), ())),
            precision=lax.Precision.HIGHEST, preferred_element_type=F32,
        )
        rides.append(row[0:1, :])
    return jnp.concatenate(rides, axis=1)


def arrived(got_ref, scatter_ref):
    flat = got_ref[...].reshape(-1, 2 * BS)
    return pick(scatter_ref[...], flat)


def ridden(got_ref):
    slots = got_ref.shape[1]
    ride = got_ref[0, slots - 1 : slots, :]
    for s in range(1, got_ref.shape[0]):
        ride = ride + got_ref[s, slots - 1 : slots, :]
    return ride


def first_kernel(got_ref, over_ref, b_ref, diag_ref, wanted_ref, scatter_ref, p_ref, out_ref, dots_ref):
    sources, slots = got_ref.shape[0], got_ref.shape[1]
    lists = jnp.concatenate([got_ref[g, slots - 1 : slots, :BS] for g in range(sources)], axis=0).T
    lane = lax.broadcasted_iota(jnp.int32, (slots, BS), 1).astype(F32)
    rows = [jnp.where(lists[:slots, g : g + 1] == lane, 1.0, 0.0) for g in range(sources)]
    scatter_ref[...] = jnp.concatenate(rows, axis=0).T.astype(BF16)
    b = b_ref[...]
    p = arrived(got_ref, scatter_ref) + jnp.concatenate([diag_ref[...]] * 2, axis=1) * b
    p_ref[...] = p
    send_out(p, wanted_ref, inner_products(dots_ref, [], b, p, 0) + over_ref[0:1, :], out_ref)


def column_of(ride, j):
    lane = lax.broadcasted_iota(jnp.int32, (1, BS), 1)
    out = []
    for n in range(2):
        row = ride[:, n * BS : (n + 1) * BS]
        inverse = 1.0 / jnp.sqrt(lane_of(row, QQ) + epsilon)
        h = row * jnp.where(lane == j, inverse * inverse, jnp.broadcast_to(inverse, (1, BS)))
        out.append((h, inverse))
    return out


def step_kernel(j, *refs):
    got_ref, scatter_ref, q_ref, p_ref, diag_ref, wanted_ref = refs[:6]
    v_refs = refs[6 : 6 + j]
    m_refs = refs[6 + j : 6 + 2 * j]
    v_ref, m_ref, q_out, p_out, ride_out, out_ref, dots_ref = refs[6 + 2 * j :]
    ride = ridden(got_ref)
    ride_out[...] = jnp.broadcast_to(ride, ride_out.shape)
    coeffs = column_of(ride, j)
    z = arrived(got_ref, scatter_ref)
    for n, (h, inverse) in enumerate(coeffs):
        cut = slice(n * BS, (n + 1) * BS)
        pn = p_ref[:, cut]
        v = q_ref[:, cut] * inverse
        m = pn * inverse
        v_ref[:, cut] = v
        m_ref[:, cut] = m
        q_next = m - lane_of(h, j) * v
        p_next = (z[:, cut] + diag_ref[...] * pn) * inverse - lane_of(h, j) * m
        for i in range(j):
            q_next = q_next - lane_of(h, i) * v_refs[i][:, cut]
            p_next = p_next - lane_of(h, i) * m_refs[i][:, cut]
        q_out[:, cut] = q_next
        p_out[:, cut] = p_next
    p = p_out[...]
    ride = inner_products(dots_ref, [r[...] for r in v_refs] + [v_ref[...]], q_out[...], p, j + 1)
    if j + 1 == STEPS - 1:
        out_ref[...] = jnp.broadcast_to(ride[:, None, :], out_ref.shape)
    else:
        send_out(p, wanted_ref, ride, out_ref)


GRAM_AT, NUMBERS_AT = 16, 24
KEPT_ROWS = 96


def rotations_kernel(*refs):
    ride_refs, kept_ref = refs[:-1], refs[-1]
    rides = [r[0:1, :] for r in ride_refs]
    per_step = [column_of(ride, j) for j, ride in enumerate(rides)]
    lane = lax.broadcasted_iota(jnp.int32, (1, BS), 1)
    known = len(rides)
    kept_ref[...] = jnp.zeros(kept_ref.shape, F32)
    for n in range(2):
        rows = [ride[:, n * BS : (n + 1) * BS] for ride in rides]
        norms = [jnp.sqrt(lane_of(row, QQ) + epsilon) for row in rows]
        inverses = [per_step[j][n][1] for j in range(known)]
        for j in range(known):
            column = jnp.where(lane <= j, per_step[j][n][0], 0.0)
            if j + 1 < known:
                column = jnp.where(lane == j + 1, norms[j + 1], column)
            kept_ref[n, j : j + 1, :] = column
            gram = pltpu.roll(rows[j], BS - GRAM, 1) * inverses[j]
            own = lane_of(rows[j], QQ) * inverses[j] * inverses[j]
            gram = jnp.where(lane < j, 2.0 * gram, 0.0)
            kept_ref[n, GRAM_AT + j : GRAM_AT + j + 1, :] = jnp.where(lane == j, own, gram)
        targets = [norms[0]] + [jnp.zeros_like(norms[0])] * known
        cosines, sines, triangle = [], [], []
        for j in range(known - 1):
            column = [lane_of(per_step[j][n][0], i) for i in range(j + 1)]
            rotate(column + [norms[j + 1]], cosines, sines, targets, triangle)
        numbers = cosines + sines + [x for column in triangle for x in column] + targets[:known]
        for at, number in enumerate(numbers):
            kept_ref[n, NUMBERS_AT + at : NUMBERS_AT + at + 1, :] = jnp.broadcast_to(number, (1, BS))


def finish_kernel(last_ref, kept_ref, q_ref, *refs):
    v_refs, (solution_ref, hessenberg_ref) = refs[:-2], refs[-2:]
    known = STEPS - 1
    ride = jnp.sum(last_ref[...], axis=0)
    lane = lax.broadcasted_iota(jnp.int32, (1, BS), 1)
    both = []
    for n, (h, inverse) in enumerate(column_of(ride, known)):
        row = ride[:, n * BS : (n + 1) * BS]
        norm = jnp.sqrt(lane_of(row, QQ) + epsilon)
        h = jnp.where(lane <= known, h, 0.0)
        gram = jnp.where(lane < known, 2.0 * pltpu.roll(row, BS - GRAM, 1) * inverse, 0.0)
        gram = jnp.where(lane == known, lane_of(row, QQ) * inverse * inverse, gram)
        table = jnp.concatenate([kept_ref[n, GRAM_AT : GRAM_AT + known, :], gram], axis=0)
        column = jnp.broadcast_to(h, (8, BS)).T[:8, :1]
        form = jnp.sum(jnp.sum(table * h * column, axis=1, keepdims=True), axis=0, keepdims=True)
        twice = 2.0 * jnp.sum(h * h, axis=1, keepdims=True)
        remainder = lane_of(row, PP) * inverse * inverse - twice + form
        final_norm = jnp.sqrt(jnp.maximum(remainder, 0.0) + epsilon)
        columns = jnp.concatenate([kept_ref[n, :known, :], jnp.where(lane == known + 1, final_norm, h)], axis=0)
        before_last = lax.broadcasted_iota(jnp.int32, columns.shape, 0) == known - 1
        columns = jnp.where(before_last & (lane == known), norm, columns)
        hessenberg_ref[n] = columns.T[: STEPS + 1, :]

        def number(at):
            return kept_ref[n, NUMBERS_AT + at : NUMBERS_AT + at + 1, :]

        cosines = [number(i) for i in range(known - 1)]
        sines = [number(known - 1 + i) for i in range(known - 1)]
        at, triangle = 2 * (known - 1), []
        for j in range(known - 1):
            triangle.append([number(at + i) for i in range(j + 1)])
            at += j + 1
        targets = [number(at + i) for i in range(known)] + [None, None]
        wide = jnp.zeros((1, BS), F32)
        previous = kept_ref[n, known - 1 : known, :]
        column = [wide + lane_of(previous, i) for i in range(known)] + [wide + norm]
        rotate(column, cosines, sines, targets, triangle)
        column = [wide + lane_of(h, i) for i in range(STEPS)] + [wide + final_norm]
        rotate(column, cosines, sines, targets, triangle)
        weights = back_substitute(triangle, targets)
        cut = slice(n * BS, (n + 1) * BS)
        acc = (weights[-1] * inverse) * q_ref[:, cut]
        for i in range(STEPS - 1):
            acc = acc + weights[i] * v_refs[i][:, cut]
        both.append(acc)
    for block in range(BS):
        row = jnp.concatenate([acc[block : block + 1, :] for acc in both], axis=0)
        solution_ref[:, block * BS : (block + 1) * BS] = row


def body(blocks, block_rows, block_cols, diagonal, right_sides):
    rows_n, cols_n = lax.axis_size(ROW), lax.axis_size(COL)
    count = blocks.shape[0]
    diag = diagonal.reshape(-1, BS)
    pitch = BS + 8

    pieces_out, q = call(
        open_kernel,
        (jax.ShapeDtypeStruct((rows_n, pitch, 2 * BS), F32), jax.ShapeDtypeStruct((BS, 2 * BS), F32)),
        (right_sides, block_cols),
        name="open",
    )
    got = swap(pieces_out, ROW)
    stored = turn_blocks(blocks)
    from_whole, spread, sums, lists, over = call(
        functools.partial(plan_kernel, rows_n, cols_n),
        (
            jax.ShapeDtypeStruct((count, rows_n * pitch), BF16),
            jax.ShapeDtypeStruct((count, rows_n * SRC_SLOTS), BF16),
            jax.ShapeDtypeStruct((cols_n * DST_SLOTS, count), BF16),
            jax.ShapeDtypeStruct((8, cols_n * DST_SLOTS), F32),
            jax.ShapeDtypeStruct((8, 2 * BS), F32),
        ),
        (block_cols, block_rows),
        name="plan",
    )

    out_shape = jax.ShapeDtypeStruct((rows_n, SRC_SLOTS, 2 * BS), F32)
    vec = jax.ShapeDtypeStruct((BS, 2 * BS), F32)
    dots = pltpu.VMEM((BS, BS), F32)

    partial, turned, wanted = first_products(got, from_whole, stored, sums, lists)
    got = swap(partial, COL)
    scatter, p, send = call(
        first_kernel,
        (jax.ShapeDtypeStruct((BS, cols_n * DST_SLOTS), BF16), vec, out_shape),
        (got, over, q, diag, wanted),
        [dots],
        name="first",
    )
    vs, ms, rides = [], [], []
    for j in range(STEPS - 1):
        got = swap(block_products(swap(send, ROW), spread, turned, sums), COL)
        last = j + 1 == STEPS - 1
        outs = (
            vec, vec, vec, vec, jax.ShapeDtypeStruct((8, 2 * BS), F32),
            jax.ShapeDtypeStruct((rows_n * cols_n, 1, 2 * BS), F32) if last else out_shape,
        )
        v, m, q, p, ride, send = call(
            functools.partial(step_kernel, j), outs, (got, scatter, q, p, diag, wanted, *vs, *ms), [dots],
            name=f"step_{j}",
        )
        vs.append(v)
        ms.append(m)
        rides.append(ride)
    final = swap(send, BOTH)
    so_far = call(
        rotations_kernel, jax.ShapeDtypeStruct((2, KEPT_ROWS, BS), F32), tuple(rides), name="rotations"
    )

    def compact(final, so_far, q, *vs):
        solution, hessenberg = call(
            finish_kernel,
            (
                jax.ShapeDtypeStruct((2, BS * BS), F32),
                jax.ShapeDtypeStruct((2, STEPS + 1, STEPS), F32),
            ),
            (final, so_far, q, *vs),
            name="finish",
        )
        return solution, hessenberg

    return lax.cond(
        rides[0][0, BS + FLAG] > 0.0,
        lambda *args: dense_cycle(*args[:5]),
        lambda *args: compact(*args[5:]),
        blocks, block_rows, block_cols, diagonal, right_sides, final, so_far, q, *vs,
    )


def solution(mesh):
    placed = (P(BOTH, None, None), P(BOTH, None), P(BOTH, None), P(BOTH), P(None, BOTH))
    return jax.shard_map(
        body, mesh=mesh, in_specs=placed, out_specs=(P(None, BOTH), P()), check_vma=False
    )
```

```python
import functools

import jax
import jax.numpy as jnp
from jax import lax
from jax.experimental import pallas as pl
from jax.experimental.pallas import tpu as pltpu
from jax.sharding import PartitionSpec as P

STEPS = 8
BS = 128
SRC_SLOTS = 56
DST_SLOTS = 24
ROW = "row"
COL = "col"
BOTH = ("row", "col")
F32 = jnp.float32
BF16 = jnp.bfloat16

epsilon = 1e-06

QQ, PP, GRAM, FLAG, PER_SYSTEM = 9, 10, 16, 31, 32


def swap(value, axis):
    return lax.all_to_all(value, axis, split_axis=0, concat_axis=0, tiled=True)


def least_squares(hessenberg, initial_norm):
    total_steps = hessenberg.shape[2]
    targets = [initial_norm] + [jnp.zeros_like(initial_norm) for j in range(total_steps)]
    cosines, sines, triangle = ([], [], [])
    for j in range(total_steps):
        column = [hessenberg[:, i, j] for i in range(j + 2)]
        rotate(column, cosines, sines, targets, triangle)
    return jnp.stack(back_substitute(triangle, targets), axis=1)


def rotate(column, cosines, sines, targets, triangle):
    j = len(column) - 2
    for i in range(j):
        leading, trailing = (column[i], column[i + 1])
        column[i] = cosines[i] * leading + sines[i] * trailing
        column[i + 1] = cosines[i] * trailing - sines[i] * leading
    radius = jnp.sqrt(column[j] * column[j] + column[j + 1] * column[j + 1])
    cosine = column[j] / radius
    sine_term = column[j + 1] / radius
    column[j] = radius
    cosines.append(cosine)
    sines.append(sine_term)
    targets[j + 1] = -sine_term * targets[j]
    targets[j] = cosine * targets[j]
    triangle.append(column[: j + 1])


def back_substitute(triangle, targets):
    total_steps = len(triangle)
    coeffs = [None] * total_steps
    for j in reversed(range(total_steps)):
        running = targets[j]
        for k in range(j + 1, total_steps):
            running = running - triangle[k][j] * coeffs[k]
        coeffs[j] = running / triangle[j][j]
    return coeffs


def dense_cycle(blocks, block_rows, block_cols, diagonal, right_sides):
    systems = right_sides.shape[0]
    groups = lax.axis_size(COL)
    length = right_sides.shape[1]
    row_count = groups * (length // BS)
    positions = jnp.arange(row_count, dtype=jnp.int32)
    onehot = (block_rows[0][None, :] == positions[:, None]).astype(F32)
    high = lax.Precision.HIGHEST

    def everywhere(value):
        return lax.psum(lax.psum(value, ROW), COL)

    def apply_matrix(vector):
        copies = jnp.broadcast_to(vector, (lax.axis_size(ROW), *vector.shape))
        gathered = jnp.moveaxis(swap(copies, ROW), 0, 1).reshape(systems, -1, BS)
        picked = jnp.take(gathered, block_cols[0], axis=1)
        products = jnp.sum(blocks[None] * picked[:, :, None, :], axis=3)
        partial = jnp.einsum("mk,nki->mni", onehot, products, precision=high)
        own = swap(partial.reshape(groups, -1, systems, BS), COL).sum(axis=0)
        return diagonal[None, :] * vector + jnp.transpose(own, (1, 0, 2)).reshape(systems, -1)

    def norm(vector):
        return jnp.sqrt(everywhere(jnp.sum(vector * vector, axis=1)) + epsilon)

    initial_norm = norm(right_sides)
    basis = jnp.zeros((STEPS + 1, systems, length), F32).at[0].set(right_sides / initial_norm[:, None])
    hessenberg = jnp.zeros((systems, STEPS + 1, STEPS), F32)

    def step(j, state):
        basis, hessenberg = state
        candidate = apply_matrix(basis[j])
        coeffs = everywhere(jnp.sum(basis * candidate[None], axis=2).T)
        candidate = candidate - jnp.sum(coeffs.T[:, :, None] * basis, axis=0)
        new_norm = norm(candidate)
        below = (jnp.arange(STEPS + 1) == j + 1).astype(F32)
        column = coeffs + below[None, :] * new_norm[:, None]
        here = (jnp.arange(STEPS) == j).astype(F32)
        hessenberg = hessenberg + column[:, :, None] * here[None, None, :]
        basis = basis.at[j + 1].set(candidate / new_norm[:, None])
        return basis, hessenberg

    basis, hessenberg = lax.fori_loop(0, STEPS, step, (basis, hessenberg))
    weights = least_squares(hessenberg, initial_norm)
    solution = jnp.sum(weights.T[:, :, None] * basis[:STEPS], axis=0)
    return solution, hessenberg


def whole(count):
    return [pl.BlockSpec(memory_space=pltpu.VMEM)] * count


def call(kernel, outs, operands, scratch=(), vmem=24 << 20, name=None):
    return pl.pallas_call(
        kernel,
        out_shape=outs,
        in_specs=whole(len(operands)),
        out_specs=jax.tree.map(lambda o: pl.BlockSpec(memory_space=pltpu.VMEM), outs),
        scratch_shapes=list(scratch),
        compiler_params=pltpu.CompilerParams(vmem_limit_bytes=vmem),
        name=name,
    )(*operands)


def pieces(value, count):
    out = []
    for _ in range(count):
        piece = value.astype(BF16)
        out.append(piece)
        value = value - piece.astype(F32)
    return out


def pick(selector, value, count=3):
    return sum(jnp.dot(selector, piece, preferred_element_type=F32) for piece in pieces(value, count))


CHUNKS = 8


def turn_kernel(blocks_ref, turned_ref, held_ref, made_ref, arrived_sem, left_sem):
    steps, per_step = held_ref.shape[0], held_ref.shape[1]
    pairs = per_step // 2

    def fetch(step):
        return pltpu.make_async_copy(
            blocks_ref.at[pl.ds(pl.multiple_of(step * per_step, per_step), per_step)],
            held_ref.at[step],
            arrived_sem.at[step],
        )

    def keep(step):
        return pltpu.make_async_copy(
            made_ref.at[step],
            turned_ref.at[pl.ds(pl.multiple_of(step * pairs, pairs), pairs)],
            left_sem.at[step],
        )

    for step in range(steps):
        fetch(step).start()

    def one(step, carry):
        fetch(step).wait()
        for pair in range(pairs):
            made_ref[step, pair] = jnp.concatenate(
                [held_ref[step, 2 * pair + half].astype(BF16).T for half in range(2)], axis=1
            )
        keep(step).start()
        return carry

    lax.fori_loop(0, steps, one, 0)
    for step in range(steps):
        keep(step).wait()


def turn_blocks(blocks, per_step=16):
    count = blocks.shape[0]
    steps = count // per_step
    return pl.pallas_call(
        turn_kernel,
        out_shape=pltpu.MemorySpace.HBM((count // 2, BS, 2 * BS), BF16),
        in_specs=[pl.BlockSpec(memory_space=pltpu.HBM)],
        out_specs=pl.BlockSpec(memory_space=pltpu.HBM),
        scratch_shapes=[
            pltpu.VMEM((steps, per_step, BS, BS), F32),
            pltpu.VMEM((steps, per_step // 2, BS, 2 * BS), BF16),
            pltpu.SemaphoreType.DMA((steps,)),
            pltpu.SemaphoreType.DMA((steps,)),
        ],
        compiler_params=pltpu.CompilerParams(vmem_limit_bytes=28 << 20),
        cost_estimate=pl.CostEstimate(flops=40_000_000, transcendentals=0, bytes_accessed=count * BS * BS * 6),
        name="turn_blocks",
    )(blocks)


def gather_sources(got_ref, spread_ref, left_ref):
    sources, slots = got_ref.shape[0], got_ref.shape[1]
    got = got_ref[...].reshape(sources * slots, 2 * BS)
    count = spread_ref.shape[0]
    for at, piece in enumerate(pieces(got, 2)):
        picked = jnp.dot(spread_ref[...], piece, preferred_element_type=F32)
        left_ref[pl.ds(2 * at, count, stride=4), :] = picked[:, :BS]
        left_ref[pl.ds(2 * at + 1, count, stride=4), :] = picked[:, BS:]


def multiply_pair(rows, turned, left_ref, prod_ref):
    upper = lax.broadcasted_iota(jnp.int32, (8, BS), 0) < 4
    both = jnp.dot(left_ref[rows, :].astype(BF16), turned, preferred_element_type=F32)
    prod_ref[rows, :] = jnp.where(upper, both[:, :BS], both[:, BS:])


def sum_targets(prod_ref, sums_ref, out_ref):
    count = sums_ref.shape[1]
    products = jnp.concatenate(
        [prod_ref[pl.ds(n, count, stride=4), :] + prod_ref[pl.ds(n + 2, count, stride=4), :] for n in range(2)],
        axis=1,
    )
    out_ref[...] = pick(sums_ref[...], products).reshape(out_ref.shape)


def first_product_kernel(
    got_ref, spread_ref, stored_ref, sums_ref, lists_ref, out_ref, turned_ref, wanted_ref, left_ref, prod_ref, sem
):
    per_chunk = stored_ref.shape[0] // CHUNKS

    def fetch(chunk):
        where = pl.ds(pl.multiple_of(chunk * per_chunk, per_chunk), per_chunk)
        return pltpu.make_async_copy(stored_ref.at[where], turned_ref.at[where], sem.at[chunk])

    for chunk in range(CHUNKS):
        fetch(chunk).start()
    gather_sources(got_ref, spread_ref, left_ref)
    asked = jnp.concatenate([got_ref[g, BS : BS + 1, :] for g in range(got_ref.shape[0])], axis=0)
    wanted_ref[...] = one_hots(asked, SRC_SLOTS).astype(BF16)

    def one(chunk, carry):
        fetch(chunk).wait()
        for k in range(per_chunk):
            pair = chunk * per_chunk + k
            multiply_pair(pl.ds(pl.multiple_of(8 * pair, 8), 8), turned_ref[pair], left_ref, prod_ref)
        return carry

    lax.fori_loop(0, CHUNKS, one, 0)
    sum_targets(prod_ref, sums_ref, out_ref)
    targets, slots = out_ref.shape[0], out_ref.shape[1]
    lists = lists_ref[0:1, :]
    for t in range(targets):
        own = pltpu.roll(lists, lists.shape[1] - t * slots, 1) if t else lists
        out_ref[t, slots - 1 : slots, :] = own[:, : 2 * BS]


def product_kernel(got_ref, spread_ref, turned_ref, sums_ref, out_ref, left_ref, prod_ref):
    gather_sources(got_ref, spread_ref, left_ref)

    def one(pair, carry):
        multiply_pair(pl.ds(pl.multiple_of(8 * pair, 8), 8), turned_ref[pair], left_ref, prod_ref)
        return carry

    lax.fori_loop(0, turned_ref.shape[0], one, 0, unroll=64)
    sum_targets(prod_ref, sums_ref, out_ref)
    slots = out_ref.shape[1]
    ride = ridden(got_ref)
    for t in range(out_ref.shape[0]):
        out_ref[t, slots - 1 : slots, :] = ride


def first_products(got, spread, stored, sums, lists):
    count = spread.shape[0]
    sources = got.shape[0]
    targets = sums.shape[0] // DST_SLOTS
    specs = whole(5)
    specs[2] = pl.BlockSpec(memory_space=pltpu.HBM)
    outs = (
        jax.ShapeDtypeStruct((targets, DST_SLOTS, 2 * BS), F32),
        jax.ShapeDtypeStruct(stored.shape, BF16),
        jax.ShapeDtypeStruct((sources * SRC_SLOTS, BS), BF16),
    )
    return pl.pallas_call(
        first_product_kernel,
        out_shape=outs,
        in_specs=specs,
        out_specs=tuple(whole(3)),
        scratch_shapes=[
            pltpu.VMEM((4 * count, BS), F32),
            pltpu.VMEM((4 * count, BS), F32),
            pltpu.SemaphoreType.DMA((CHUNKS,)),
        ],
        compiler_params=pltpu.CompilerParams(vmem_limit_bytes=24 << 20),
        name="first_products",
    )(got, spread, pltpu.with_memory_space_constraint(stored, pltpu.HBM), sums, lists)


def block_products(got, spread, turned, sums):
    count = spread.shape[0]
    targets = sums.shape[0] // DST_SLOTS
    return call(
        product_kernel,
        jax.ShapeDtypeStruct((targets, DST_SLOTS, 2 * BS), F32),
        (got, spread, turned, sums),
        [pltpu.VMEM((4 * count, BS), F32), pltpu.VMEM((4 * count, BS), F32)],
        vmem=16 << 20,
        name="block_products",
    )


def lane_of(row, lane):
    return row[:, lane : lane + 1]


def total(value):
    return jnp.sum(value, axis=0, keepdims=True)


def send_out(values, wanted_ref, ride, out_ref):
    out = pick(wanted_ref[...], values)
    out_ref[...] = out.reshape(out_ref.shape)
    slots = out_ref.shape[1]
    for s in range(out_ref.shape[0]):
        out_ref[s, slots - 1 : slots, :] = ride


def ranks(present):
    shape = (BS, BS)
    before = lax.broadcasted_iota(jnp.int32, shape, 0) < lax.broadcasted_iota(jnp.int32, shape, 1)
    return jnp.dot(present.astype(BF16), before.astype(F32).astype(BF16), preferred_element_type=F32)


def present_in(column, offset):
    lane = lax.broadcasted_iota(jnp.int32, (column.shape[0], BS), 1).astype(F32) + offset
    return jnp.max(jnp.where(column == lane, 1.0, 0.0), axis=0, keepdims=True)


def slot_rows(present, rank, slots, usable):
    at = lax.broadcasted_iota(jnp.int32, (slots, BS), 0).astype(F32)
    return jnp.where((rank == at) & (present > 0.0) & (at < usable), 1.0, 0.0)


def one_hots(lists, slots):
    columns = lists.T
    present = jnp.concatenate([present_in(columns[:, g : g + 1], 0.0) for g in range(lists.shape[0])], axis=0)
    rank = ranks(present)
    return jnp.concatenate(
        [slot_rows(present[g : g + 1], rank[g : g + 1], slots, slots - 1.0) for g in range(lists.shape[0])], axis=0
    )


def plan_kernel(sources, targets, cols_ref, rows_ref, whole_ref, spread_ref, sums_ref, lists_ref, over_ref):
    count = cols_ref.shape[1]

    def column_of_blocks(ref):
        return jnp.broadcast_to(ref[...].astype(F32), (8, count)).T[:, :1]

    def present_and_rank(column, groups):
        present = jnp.concatenate([present_in(column, float(g * BS)) for g in range(groups)], axis=0)
        return present, ranks(present)

    def slot_column(column, rank, groups, slots):
        lane = lax.broadcasted_iota(jnp.int32, (count, BS), 1).astype(F32)
        found = jnp.zeros(lane.shape, F32)
        for g in range(groups):
            found = found + jnp.where(column == lane + float(g * BS), rank[g : g + 1] + float(g * slots), 0.0)
        return jnp.sum(found, axis=1, keepdims=True)

    def most(present):
        return jnp.max(jnp.sum(present, axis=1, keepdims=True), axis=0, keepdims=True)

    column = column_of_blocks(cols_ref)
    present, rank = present_and_rank(column, sources)
    slot = slot_column(column, rank, sources, SRC_SLOTS)
    at = lax.broadcasted_iota(jnp.int32, spread_ref.shape, 1).astype(F32)
    spread_ref[...] = jnp.where(slot == at, 1.0, 0.0).astype(BF16)
    pitch = whole_ref.shape[1] // sources
    at = lax.broadcasted_iota(jnp.int32, (count, pitch), 1).astype(F32)
    in_group = jnp.concatenate(
        [jnp.where((column - float(g * BS) == at) & (at < BS), 1.0, 0.0) for g in range(sources)], axis=1
    )
    whole_ref[...] = in_group.astype(BF16)
    over = most(present) > SRC_SLOTS - 1.0

    column = column_of_blocks(rows_ref)
    present, rank = present_and_rank(column, targets)
    slot = slot_column(column, rank, targets, DST_SLOTS)
    row = jnp.broadcast_to(slot, (count, BS)).T[:1, :]
    at = lax.broadcasted_iota(jnp.int32, sums_ref.shape, 0).astype(F32)
    sums_ref[...] = jnp.where(row == at, 1.0, 0.0).astype(BF16)
    listed = jnp.concatenate(
        [slot_rows(present[t : t + 1], rank[t : t + 1], DST_SLOTS, DST_SLOTS - 1.0) for t in range(targets)], axis=0
    )
    number = lax.broadcasted_iota(jnp.int32, (8, BS), 1).astype(F32) + 1.0
    lists_ref[...] = lax.dot_general(
        number.astype(BF16), listed.astype(BF16), (((1,), (1,)), ((), ())), preferred_element_type=F32
    ) - 1.0
    over = jnp.where(over | (most(present) > DST_SLOTS - 1.0), 1.0, 0.0)
    lane = lax.broadcasted_iota(jnp.int32, over_ref.shape, 1)
    over_ref[...] = jnp.where(lane == FLAG, over, 0.0)


def open_kernel(sides_ref, cols_ref, out_ref, b_ref):
    for at in range(0, BS, 8):
        tiles = [sides_ref[:, (at + k) * BS : (at + k + 1) * BS] for k in range(8)]
        for n in range(2):
            b_ref[at : at + 8, n * BS : (n + 1) * BS] = jnp.concatenate([t[n : n + 1, :] for t in tiles], axis=0)
    below = lax.broadcasted_iota(jnp.int32, (8, 2 * BS), 0) == 0
    cols = cols_ref[...].astype(F32)
    for g in range(out_ref.shape[0]):
        out_ref[g, :BS, :] = b_ref[...]
        out_ref[g, BS:, :] = jnp.where(below, cols - float(g * BS), 0.0)


def inner_products(dots_ref, vs, q, p, j):
    dots_ref[...] = jnp.zeros(dots_ref.shape, F32)
    for n in range(2):
        cut = slice(n * BS, (n + 1) * BS)
        base = n * PER_SYSTEM
        qn, pn = q[:, cut], p[:, cut]
        for i in range(j):
            vn = vs[i][:, cut]
            dots_ref[base + i : base + i + 1, :] = total(vn * pn)
            dots_ref[base + GRAM + i : base + GRAM + i + 1, :] = total(vn * qn)
        dots_ref[base + j : base + j + 1, :] = total(qn * pn)
        dots_ref[base + QQ : base + QQ + 1, :] = total(qn * qn)
        dots_ref[base + PP : base + PP + 1, :] = total(pn * pn)
    row = lax.dot_general(
        jnp.ones((8, BS), F32), dots_ref[...], (((1,), (1,)), ((), ())),
        precision=lax.Precision.HIGHEST, preferred_element_type=F32,
    )[0:1, :]
    return jnp.concatenate([row, jnp.zeros((1, BS - row.shape[1]), F32)], axis=1)


def system_row(ride, n):
    row = ride[:, :BS]
    return pltpu.roll(row, BS - n * PER_SYSTEM, 1) if n else row


def widened(row):
    return jnp.concatenate([row, jnp.zeros_like(row)], axis=1)


def arrived(got_ref, scatter_ref):
    flat = got_ref[...].reshape(-1, 2 * BS)
    return pick(scatter_ref[...], flat)


def ridden(got_ref):
    slots = got_ref.shape[1]
    ride = got_ref[0, slots - 1 : slots, :]
    for s in range(1, got_ref.shape[0]):
        ride = ride + got_ref[s, slots - 1 : slots, :]
    return ride


def first_kernel(got_ref, over_ref, b_ref, diag_ref, wanted_ref, scatter_ref, p_ref, out_ref, dots_ref):
    sources, slots = got_ref.shape[0], got_ref.shape[1]
    lists = jnp.concatenate([got_ref[g, slots - 1 : slots, :BS] for g in range(sources)], axis=0).T
    lane = lax.broadcasted_iota(jnp.int32, (slots, BS), 1).astype(F32)
    rows = [jnp.where(lists[:slots, g : g + 1] == lane, 1.0, 0.0) for g in range(sources)]
    scatter_ref[...] = jnp.concatenate(rows, axis=0).T.astype(BF16)
    b = b_ref[...]
    p = arrived(got_ref, scatter_ref) + jnp.concatenate([diag_ref[...]] * 2, axis=1) * b
    p_ref[...] = p
    send_out(p, wanted_ref, widened(inner_products(dots_ref, [], b, p, 0)) + over_ref[0:1, :], out_ref)


def column_of(ride, j):
    lane = lax.broadcasted_iota(jnp.int32, (1, BS), 1)
    out = []
    for n in range(2):
        row = system_row(ride, n)
        inverse = 1.0 / jnp.sqrt(lane_of(row, QQ) + epsilon)
        h = row * jnp.where(lane == j, inverse * inverse, jnp.broadcast_to(inverse, (1, BS)))
        out.append((h, inverse))
    return out


def step_kernel(j, *refs):
    got_ref, scatter_ref, q_ref, p_ref, diag_ref, wanted_ref = refs[:6]
    v_refs = refs[6 : 6 + j]
    m_refs = refs[6 + j : 6 + 2 * j]
    v_ref, m_ref, q_out, p_out, ride_out, out_ref, dots_ref = refs[6 + 2 * j :]
    ride = ridden(got_ref)
    ride_out[...] = jnp.broadcast_to(ride, ride_out.shape)
    coeffs = column_of(ride, j)
    z = arrived(got_ref, scatter_ref)
    for n, (h, inverse) in enumerate(coeffs):
        cut = slice(n * BS, (n + 1) * BS)
        pn = p_ref[:, cut]
        v = q_ref[:, cut] * inverse
        m = pn * inverse
        v_ref[:, cut] = v
        m_ref[:, cut] = m
        q_next = m - lane_of(h, j) * v
        p_next = (z[:, cut] + diag_ref[...] * pn) * inverse - lane_of(h, j) * m
        for i in range(j):
            q_next = q_next - lane_of(h, i) * v_refs[i][:, cut]
            p_next = p_next - lane_of(h, i) * m_refs[i][:, cut]
        q_out[:, cut] = q_next
        p_out[:, cut] = p_next
    p = p_out[...]
    ride = inner_products(dots_ref, [r[...] for r in v_refs] + [v_ref[...]], q_out[...], p, j + 1)
    if j + 1 == STEPS - 1:
        out_ref[...] = jnp.broadcast_to(ride[:, None, :], out_ref.shape)
    else:
        send_out(p, wanted_ref, widened(ride), out_ref)


GRAM_AT, NUMBERS_AT = 16, 24
KEPT_ROWS = 96


def rotations_kernel(*refs):
    ride_refs, kept_ref = refs[:-1], refs[-1]
    rides = [r[0:1, :] for r in ride_refs]
    per_step = [column_of(ride, j) for j, ride in enumerate(rides)]
    lane = lax.broadcasted_iota(jnp.int32, (1, BS), 1)
    known = len(rides)
    kept_ref[...] = jnp.zeros(kept_ref.shape, F32)
    for n in range(2):
        rows = [system_row(ride, n) for ride in rides]
        norms = [jnp.sqrt(lane_of(row, QQ) + epsilon) for row in rows]
        inverses = [per_step[j][n][1] for j in range(known)]
        for j in range(known):
            column = jnp.where(lane <= j, per_step[j][n][0], 0.0)
            if j + 1 < known:
                column = jnp.where(lane == j + 1, norms[j + 1], column)
            kept_ref[n, j : j + 1, :] = column
            gram = pltpu.roll(rows[j], BS - GRAM, 1) * inverses[j]
            own = lane_of(rows[j], QQ) * inverses[j] * inverses[j]
            gram = jnp.where(lane < j, 2.0 * gram, 0.0)
            kept_ref[n, GRAM_AT + j : GRAM_AT + j + 1, :] = jnp.where(lane == j, own, gram)
        targets = [norms[0]] + [jnp.zeros_like(norms[0])] * known
        cosines, sines, triangle = [], [], []
        for j in range(known - 1):
            column = [lane_of(per_step[j][n][0], i) for i in range(j + 1)]
            rotate(column + [norms[j + 1]], cosines, sines, targets, triangle)
        numbers = cosines + sines + [x for column in triangle for x in column] + targets[:known]
        for at, number in enumerate(numbers):
            kept_ref[n, NUMBERS_AT + at : NUMBERS_AT + at + 1, :] = jnp.broadcast_to(number, (1, BS))


def finish_kernel(last_ref, kept_ref, q_ref, *refs):
    v_refs, (solution_ref, hessenberg_ref) = refs[:-2], refs[-2:]
    known = STEPS - 1
    ride = jnp.sum(last_ref[...], axis=0)
    lane = lax.broadcasted_iota(jnp.int32, (1, BS), 1)
    both = []
    for n, (h, inverse) in enumerate(column_of(ride, known)):
        row = system_row(ride, n)
        norm = jnp.sqrt(lane_of(row, QQ) + epsilon)
        h = jnp.where(lane <= known, h, 0.0)
        gram = jnp.where(lane < known, 2.0 * pltpu.roll(row, BS - GRAM, 1) * inverse, 0.0)
        gram = jnp.where(lane == known, lane_of(row, QQ) * inverse * inverse, gram)
        table = jnp.concatenate([kept_ref[n, GRAM_AT : GRAM_AT + known, :], gram], axis=0)
        column = jnp.broadcast_to(h, (8, BS)).T[:8, :1]
        form = jnp.sum(jnp.sum(table * h * column, axis=1, keepdims=True), axis=0, keepdims=True)
        twice = 2.0 * jnp.sum(h * h, axis=1, keepdims=True)
        remainder = lane_of(row, PP) * inverse * inverse - twice + form
        final_norm = jnp.sqrt(jnp.maximum(remainder, 0.0) + epsilon)
        columns = jnp.concatenate([kept_ref[n, :known, :], jnp.where(lane == known + 1, final_norm, h)], axis=0)
        before_last = lax.broadcasted_iota(jnp.int32, columns.shape, 0) == known - 1
        columns = jnp.where(before_last & (lane == known), norm, columns)
        hessenberg_ref[n] = columns.T[: STEPS + 1, :]

        def number(at):
            return kept_ref[n, NUMBERS_AT + at : NUMBERS_AT + at + 1, :]

        cosines = [number(i) for i in range(known - 1)]
        sines = [number(known - 1 + i) for i in range(known - 1)]
        at, triangle = 2 * (known - 1), []
        for j in range(known - 1):
            triangle.append([number(at + i) for i in range(j + 1)])
            at += j + 1
        targets = [number(at + i) for i in range(known)] + [None, None]
        wide = jnp.zeros((1, BS), F32)
        previous = kept_ref[n, known - 1 : known, :]
        column = [wide + lane_of(previous, i) for i in range(known)] + [wide + norm]
        rotate(column, cosines, sines, targets, triangle)
        column = [wide + lane_of(h, i) for i in range(STEPS)] + [wide + final_norm]
        rotate(column, cosines, sines, targets, triangle)
        weights = back_substitute(triangle, targets)
        cut = slice(n * BS, (n + 1) * BS)
        acc = (weights[-1] * inverse) * q_ref[:, cut]
        for i in range(STEPS - 1):
            acc = acc + weights[i] * v_refs[i][:, cut]
        both.append(acc)
    for block in range(BS):
        row = jnp.concatenate([acc[block : block + 1, :] for acc in both], axis=0)
        solution_ref[:, block * BS : (block + 1) * BS] = row


def body(blocks, block_rows, block_cols, diagonal, right_sides):
    rows_n, cols_n = lax.axis_size(ROW), lax.axis_size(COL)
    count = blocks.shape[0]
    diag = diagonal.reshape(-1, BS)
    pitch = BS + 8

    pieces_out, q = call(
        open_kernel,
        (jax.ShapeDtypeStruct((rows_n, pitch, 2 * BS), F32), jax.ShapeDtypeStruct((BS, 2 * BS), F32)),
        (right_sides, block_cols),
        name="open",
    )
    got = swap(pieces_out, ROW)
    stored = turn_blocks(blocks)
    from_whole, spread, sums, lists, over = call(
        functools.partial(plan_kernel, rows_n, cols_n),
        (
            jax.ShapeDtypeStruct((count, rows_n * pitch), BF16),
            jax.ShapeDtypeStruct((count, rows_n * SRC_SLOTS), BF16),
            jax.ShapeDtypeStruct((cols_n * DST_SLOTS, count), BF16),
            jax.ShapeDtypeStruct((8, cols_n * DST_SLOTS), F32),
            jax.ShapeDtypeStruct((8, 2 * BS), F32),
        ),
        (block_cols, block_rows),
        name="plan",
    )

    out_shape = jax.ShapeDtypeStruct((rows_n, SRC_SLOTS, 2 * BS), F32)
    vec = jax.ShapeDtypeStruct((BS, 2 * BS), F32)
    dots = pltpu.VMEM((2 * PER_SYSTEM, BS), F32)

    partial, turned, wanted = first_products(got, from_whole, stored, sums, lists)
    got = swap(partial, COL)
    scatter, p, send = call(
        first_kernel,
        (jax.ShapeDtypeStruct((BS, cols_n * DST_SLOTS), BF16), vec, out_shape),
        (got, over, q, diag, wanted),
        [dots],
        name="first",
    )
    vs, ms, rides = [], [], []
    for j in range(STEPS - 1):
        got = swap(block_products(swap(send, ROW), spread, turned, sums), COL)
        last = j + 1 == STEPS - 1
        outs = (
            vec, vec, vec, vec, jax.ShapeDtypeStruct((8, 2 * BS), F32),
            jax.ShapeDtypeStruct((rows_n * cols_n, 1, BS), F32) if last else out_shape,
        )
        v, m, q, p, ride, send = call(
            functools.partial(step_kernel, j), outs, (got, scatter, q, p, diag, wanted, *vs, *ms), [dots],
            name=f"step_{j}",
        )
        vs.append(v)
        ms.append(m)
        rides.append(ride)
    final = swap(send, BOTH)
    so_far = call(
        rotations_kernel, jax.ShapeDtypeStruct((2, KEPT_ROWS, BS), F32), tuple(rides), name="rotations"
    )

    def compact(final, so_far, q, *vs):
        solution, hessenberg = call(
            finish_kernel,
            (
                jax.ShapeDtypeStruct((2, BS * BS), F32),
                jax.ShapeDtypeStruct((2, STEPS + 1, STEPS), F32),
            ),
            (final, so_far, q, *vs),
            name="finish",
        )
        return solution, hessenberg

    return lax.cond(
        rides[0][0, FLAG] > 0.0,
        lambda *args: dense_cycle(*args[:5]),
        lambda *args: compact(*args[5:]),
        blocks, block_rows, block_cols, diagonal, right_sides, final, so_far, q, *vs,
    )


def solution(mesh):
    placed = (P(BOTH, None, None), P(BOTH, None), P(BOTH, None), P(BOTH), P(None, BOTH))
    return jax.shard_map(
        body, mesh=mesh, in_specs=placed, out_specs=(P(None, BOTH), P()), check_vma=False
    )
```

```python
import functools

import jax
import jax.numpy as jnp
from jax import lax
from jax.experimental import pallas as pl
from jax.experimental.pallas import tpu as pltpu
from jax.sharding import PartitionSpec as P

STEPS = 8
BS = 128
SRC_SLOTS = 56
DST_SLOTS = 24
ROW = "row"
COL = "col"
BOTH = ("row", "col")
F32 = jnp.float32
BF16 = jnp.bfloat16

epsilon = 1e-06

QQ, PP, GRAM, FLAG, PER_SYSTEM = 9, 10, 16, 31, 32


def swap(value, axis):
    return lax.all_to_all(value, axis, split_axis=0, concat_axis=0, tiled=True)


def least_squares(hessenberg, initial_norm):
    total_steps = hessenberg.shape[2]
    targets = [initial_norm] + [jnp.zeros_like(initial_norm) for j in range(total_steps)]
    cosines, sines, triangle = ([], [], [])
    for j in range(total_steps):
        column = [hessenberg[:, i, j] for i in range(j + 2)]
        rotate(column, cosines, sines, targets, triangle)
    return jnp.stack(back_substitute(triangle, targets), axis=1)


def rotate(column, cosines, sines, targets, triangle):
    j = len(column) - 2
    for i in range(j):
        leading, trailing = (column[i], column[i + 1])
        column[i] = cosines[i] * leading + sines[i] * trailing
        column[i + 1] = cosines[i] * trailing - sines[i] * leading
    radius = jnp.sqrt(column[j] * column[j] + column[j + 1] * column[j + 1])
    cosine = column[j] / radius
    sine_term = column[j + 1] / radius
    column[j] = radius
    cosines.append(cosine)
    sines.append(sine_term)
    targets[j + 1] = -sine_term * targets[j]
    targets[j] = cosine * targets[j]
    triangle.append(column[: j + 1])


def back_substitute(triangle, targets):
    total_steps = len(triangle)
    coeffs = [None] * total_steps
    for j in reversed(range(total_steps)):
        running = targets[j]
        for k in range(j + 1, total_steps):
            running = running - triangle[k][j] * coeffs[k]
        coeffs[j] = running / triangle[j][j]
    return coeffs


def dense_cycle(blocks, block_rows, block_cols, diagonal, right_sides):
    systems = right_sides.shape[0]
    groups = lax.axis_size(COL)
    length = right_sides.shape[1]
    row_count = groups * (length // BS)
    positions = jnp.arange(row_count, dtype=jnp.int32)
    onehot = (block_rows[0][None, :] == positions[:, None]).astype(F32)
    high = lax.Precision.HIGHEST

    def everywhere(value):
        return lax.psum(lax.psum(value, ROW), COL)

    def apply_matrix(vector):
        copies = jnp.broadcast_to(vector, (lax.axis_size(ROW), *vector.shape))
        gathered = jnp.moveaxis(swap(copies, ROW), 0, 1).reshape(systems, -1, BS)
        picked = jnp.take(gathered, block_cols[0], axis=1)
        products = jnp.sum(blocks[None] * picked[:, :, None, :], axis=3)
        partial = jnp.einsum("mk,nki->mni", onehot, products, precision=high)
        own = swap(partial.reshape(groups, -1, systems, BS), COL).sum(axis=0)
        return diagonal[None, :] * vector + jnp.transpose(own, (1, 0, 2)).reshape(systems, -1)

    def norm(vector):
        return jnp.sqrt(everywhere(jnp.sum(vector * vector, axis=1)) + epsilon)

    initial_norm = norm(right_sides)
    basis = jnp.zeros((STEPS + 1, systems, length), F32).at[0].set(right_sides / initial_norm[:, None])
    hessenberg = jnp.zeros((systems, STEPS + 1, STEPS), F32)

    def step(j, state):
        basis, hessenberg = state
        candidate = apply_matrix(basis[j])
        coeffs = everywhere(jnp.sum(basis * candidate[None], axis=2).T)
        candidate = candidate - jnp.sum(coeffs.T[:, :, None] * basis, axis=0)
        new_norm = norm(candidate)
        below = (jnp.arange(STEPS + 1) == j + 1).astype(F32)
        column = coeffs + below[None, :] * new_norm[:, None]
        here = (jnp.arange(STEPS) == j).astype(F32)
        hessenberg = hessenberg + column[:, :, None] * here[None, None, :]
        basis = basis.at[j + 1].set(candidate / new_norm[:, None])
        return basis, hessenberg

    basis, hessenberg = lax.fori_loop(0, STEPS, step, (basis, hessenberg))
    weights = least_squares(hessenberg, initial_norm)
    solution = jnp.sum(weights.T[:, :, None] * basis[:STEPS], axis=0)
    return solution, hessenberg


def whole(count):
    return [pl.BlockSpec(memory_space=pltpu.VMEM)] * count


def call(kernel, outs, operands, scratch=(), vmem=24 << 20, name=None):
    return pl.pallas_call(
        kernel,
        out_shape=outs,
        in_specs=whole(len(operands)),
        out_specs=jax.tree.map(lambda o: pl.BlockSpec(memory_space=pltpu.VMEM), outs),
        scratch_shapes=list(scratch),
        compiler_params=pltpu.CompilerParams(vmem_limit_bytes=vmem),
        name=name,
    )(*operands)


def pieces(value, count):
    out = []
    for _ in range(count):
        piece = value.astype(BF16)
        out.append(piece)
        value = value - piece.astype(F32)
    return out


def pick(selector, value, count=3):
    return sum(jnp.dot(selector, piece, preferred_element_type=F32) for piece in pieces(value, count))


CHUNKS = 8


def turn_kernel(blocks_ref, turned_ref, held_ref, made_ref, arrived_sem, left_sem):
    steps, per_step = held_ref.shape[0], held_ref.shape[1]
    pairs = per_step // 2

    def fetch(step):
        return pltpu.make_async_copy(
            blocks_ref.at[pl.ds(pl.multiple_of(step * per_step, per_step), per_step)],
            held_ref.at[step],
            arrived_sem.at[step],
        )

    def keep(step):
        return pltpu.make_async_copy(
            made_ref.at[step],
            turned_ref.at[pl.ds(pl.multiple_of(step * pairs, pairs), pairs)],
            left_sem.at[step],
        )

    for step in range(steps):
        fetch(step).start()

    def one(step, carry):
        fetch(step).wait()
        for pair in range(pairs):
            made_ref[step, pair] = jnp.concatenate(
                [held_ref[step, 2 * pair + half].astype(BF16).T for half in range(2)], axis=1
            )
        keep(step).start()
        return carry

    lax.fori_loop(0, steps, one, 0)
    for step in range(steps):
        keep(step).wait()


def turn_blocks(blocks, per_step=16):
    count = blocks.shape[0]
    steps = count // per_step
    return pl.pallas_call(
        turn_kernel,
        out_shape=pltpu.MemorySpace.HBM((count // 2, BS, 2 * BS), BF16),
        in_specs=[pl.BlockSpec(memory_space=pltpu.HBM)],
        out_specs=pl.BlockSpec(memory_space=pltpu.HBM),
        scratch_shapes=[
            pltpu.VMEM((steps, per_step, BS, BS), F32),
            pltpu.VMEM((steps, per_step // 2, BS, 2 * BS), BF16),
            pltpu.SemaphoreType.DMA((steps,)),
            pltpu.SemaphoreType.DMA((steps,)),
        ],
        compiler_params=pltpu.CompilerParams(vmem_limit_bytes=28 << 20),
        cost_estimate=pl.CostEstimate(flops=40_000_000, transcendentals=0, bytes_accessed=count * BS * BS * 6),
        name="turn_blocks",
    )(blocks)


def gather_sources(got_ref, spread_ref, left_ref):
    sources, slots = got_ref.shape[0], got_ref.shape[1]
    got = got_ref[...].reshape(sources * slots, 2 * BS)
    count = spread_ref.shape[0]
    for at, piece in enumerate(pieces(got, 2)):
        picked = jnp.dot(spread_ref[...], piece, preferred_element_type=F32)
        left_ref[pl.ds(2 * at, count, stride=4), :] = picked[:, :BS]
        left_ref[pl.ds(2 * at + 1, count, stride=4), :] = picked[:, BS:]


def multiply_pair(rows, turned, left_ref, prod_ref):
    upper = lax.broadcasted_iota(jnp.int32, (8, BS), 0) < 4
    both = jnp.dot(left_ref[rows, :].astype(BF16), turned, preferred_element_type=F32)
    prod_ref[rows, :] = jnp.where(upper, both[:, :BS], both[:, BS:])


def sum_targets(prod_ref, sums_ref, out_ref):
    count = sums_ref.shape[1]
    products = jnp.concatenate(
        [prod_ref[pl.ds(n, count, stride=4), :] + prod_ref[pl.ds(n + 2, count, stride=4), :] for n in range(2)],
        axis=1,
    )
    out_ref[...] = pick(sums_ref[...], products, 2).reshape(out_ref.shape)


def first_product_kernel(
    got_ref, spread_ref, stored_ref, sums_ref, lists_ref, out_ref, turned_ref, wanted_ref, left_ref, prod_ref, sem
):
    per_chunk = stored_ref.shape[0] // CHUNKS

    def fetch(chunk):
        where = pl.ds(pl.multiple_of(chunk * per_chunk, per_chunk), per_chunk)
        return pltpu.make_async_copy(stored_ref.at[where], turned_ref.at[where], sem.at[chunk])

    for chunk in range(CHUNKS):
        fetch(chunk).start()
    gather_sources(got_ref, spread_ref, left_ref)
    asked = jnp.concatenate([got_ref[g, BS : BS + 1, :] for g in range(got_ref.shape[0])], axis=0)
    wanted_ref[...] = one_hots(asked, SRC_SLOTS).astype(BF16)

    def one(chunk, carry):
        fetch(chunk).wait()
        for k in range(per_chunk):
            pair = chunk * per_chunk + k
            multiply_pair(pl.ds(pl.multiple_of(8 * pair, 8), 8), turned_ref[pair], left_ref, prod_ref)
        return carry

    lax.fori_loop(0, CHUNKS, one, 0)
    sum_targets(prod_ref, sums_ref, out_ref)
    targets, slots = out_ref.shape[0], out_ref.shape[1]
    lists = lists_ref[0:1, :]
    for t in range(targets):
        own = pltpu.roll(lists, lists.shape[1] - t * slots, 1) if t else lists
        out_ref[t, slots - 1 : slots, :] = own[:, : 2 * BS]


def product_kernel(got_ref, spread_ref, turned_ref, sums_ref, out_ref, left_ref, prod_ref):
    gather_sources(got_ref, spread_ref, left_ref)

    def one(pair, carry):
        multiply_pair(pl.ds(pl.multiple_of(8 * pair, 8), 8), turned_ref[pair], left_ref, prod_ref)
        return carry

    lax.fori_loop(0, turned_ref.shape[0], one, 0, unroll=64)
    sum_targets(prod_ref, sums_ref, out_ref)
    slots = out_ref.shape[1]
    ride = ridden(got_ref)
    for t in range(out_ref.shape[0]):
        out_ref[t, slots - 1 : slots, :] = ride


def first_products(got, spread, stored, sums, lists):
    count = spread.shape[0]
    sources = got.shape[0]
    targets = sums.shape[0] // DST_SLOTS
    specs = whole(5)
    specs[2] = pl.BlockSpec(memory_space=pltpu.HBM)
    outs = (
        jax.ShapeDtypeStruct((targets, DST_SLOTS, 2 * BS), F32),
        jax.ShapeDtypeStruct(stored.shape, BF16),
        jax.ShapeDtypeStruct((sources * SRC_SLOTS, BS), BF16),
    )
    return pl.pallas_call(
        first_product_kernel,
        out_shape=outs,
        in_specs=specs,
        out_specs=tuple(whole(3)),
        scratch_shapes=[
            pltpu.VMEM((4 * count, BS), F32),
            pltpu.VMEM((4 * count, BS), F32),
            pltpu.SemaphoreType.DMA((CHUNKS,)),
        ],
        compiler_params=pltpu.CompilerParams(vmem_limit_bytes=24 << 20),
        name="first_products",
    )(got, spread, pltpu.with_memory_space_constraint(stored, pltpu.HBM), sums, lists)


def block_products(got, spread, turned, sums):
    count = spread.shape[0]
    targets = sums.shape[0] // DST_SLOTS
    return call(
        product_kernel,
        jax.ShapeDtypeStruct((targets, DST_SLOTS, 2 * BS), F32),
        (got, spread, turned, sums),
        [pltpu.VMEM((4 * count, BS), F32), pltpu.VMEM((4 * count, BS), F32)],
        vmem=16 << 20,
        name="block_products",
    )


def lane_of(row, lane):
    return row[:, lane : lane + 1]


def total(value):
    return jnp.sum(value, axis=0, keepdims=True)


def send_out(values, wanted_ref, ride, out_ref):
    out = pick(wanted_ref[...], values)
    out_ref[...] = out.reshape(out_ref.shape)
    slots = out_ref.shape[1]
    for s in range(out_ref.shape[0]):
        out_ref[s, slots - 1 : slots, :] = ride


def ranks(present):
    shape = (BS, BS)
    before = lax.broadcasted_iota(jnp.int32, shape, 0) < lax.broadcasted_iota(jnp.int32, shape, 1)
    return jnp.dot(present.astype(BF16), before.astype(F32).astype(BF16), preferred_element_type=F32)


def present_in(column, offset):
    lane = lax.broadcasted_iota(jnp.int32, (column.shape[0], BS), 1).astype(F32) + offset
    return jnp.max(jnp.where(column == lane, 1.0, 0.0), axis=0, keepdims=True)


def slot_rows(present, rank, slots, usable):
    at = lax.broadcasted_iota(jnp.int32, (slots, BS), 0).astype(F32)
    return jnp.where((rank == at) & (present > 0.0) & (at < usable), 1.0, 0.0)


def one_hots(lists, slots):
    columns = lists.T
    present = jnp.concatenate([present_in(columns[:, g : g + 1], 0.0) for g in range(lists.shape[0])], axis=0)
    rank = ranks(present)
    return jnp.concatenate(
        [slot_rows(present[g : g + 1], rank[g : g + 1], slots, slots - 1.0) for g in range(lists.shape[0])], axis=0
    )


def plan_kernel(sources, targets, cols_ref, rows_ref, whole_ref, spread_ref, sums_ref, lists_ref, over_ref):
    count = cols_ref.shape[1]

    def column_of_blocks(ref):
        return jnp.broadcast_to(ref[...].astype(F32), (8, count)).T[:, :1]

    def present_and_rank(column, groups):
        present = jnp.concatenate([present_in(column, float(g * BS)) for g in range(groups)], axis=0)
        return present, ranks(present)

    def slot_column(column, rank, groups, slots):
        lane = lax.broadcasted_iota(jnp.int32, (count, BS), 1).astype(F32)
        found = jnp.zeros(lane.shape, F32)
        for g in range(groups):
            found = found + jnp.where(column == lane + float(g * BS), rank[g : g + 1] + float(g * slots), 0.0)
        return jnp.sum(found, axis=1, keepdims=True)

    def most(present):
        return jnp.max(jnp.sum(present, axis=1, keepdims=True), axis=0, keepdims=True)

    column = column_of_blocks(cols_ref)
    present, rank = present_and_rank(column, sources)
    slot = slot_column(column, rank, sources, SRC_SLOTS)
    at = lax.broadcasted_iota(jnp.int32, spread_ref.shape, 1).astype(F32)
    spread_ref[...] = jnp.where(slot == at, 1.0, 0.0).astype(BF16)
    pitch = whole_ref.shape[1] // sources
    at = lax.broadcasted_iota(jnp.int32, (count, pitch), 1).astype(F32)
    in_group = jnp.concatenate(
        [jnp.where((column - float(g * BS) == at) & (at < BS), 1.0, 0.0) for g in range(sources)], axis=1
    )
    whole_ref[...] = in_group.astype(BF16)
    over = most(present) > SRC_SLOTS - 1.0

    column = column_of_blocks(rows_ref)
    present, rank = present_and_rank(column, targets)
    slot = slot_column(column, rank, targets, DST_SLOTS)
    row = jnp.broadcast_to(slot, (count, BS)).T[:1, :]
    at = lax.broadcasted_iota(jnp.int32, sums_ref.shape, 0).astype(F32)
    sums_ref[...] = jnp.where(row == at, 1.0, 0.0).astype(BF16)
    listed = jnp.concatenate(
        [slot_rows(present[t : t + 1], rank[t : t + 1], DST_SLOTS, DST_SLOTS - 1.0) for t in range(targets)], axis=0
    )
    number = lax.broadcasted_iota(jnp.int32, (8, BS), 1).astype(F32) + 1.0
    lists_ref[...] = lax.dot_general(
        number.astype(BF16), listed.astype(BF16), (((1,), (1,)), ((), ())), preferred_element_type=F32
    ) - 1.0
    over = jnp.where(over | (most(present) > DST_SLOTS - 1.0), 1.0, 0.0)
    lane = lax.broadcasted_iota(jnp.int32, over_ref.shape, 1)
    over_ref[...] = jnp.where(lane == FLAG, over, 0.0)


def open_kernel(sides_ref, cols_ref, out_ref, b_ref):
    for at in range(0, BS, 8):
        tiles = [sides_ref[:, (at + k) * BS : (at + k + 1) * BS] for k in range(8)]
        for n in range(2):
            b_ref[at : at + 8, n * BS : (n + 1) * BS] = jnp.concatenate([t[n : n + 1, :] for t in tiles], axis=0)
    below = lax.broadcasted_iota(jnp.int32, (8, 2 * BS), 0) == 0
    cols = cols_ref[...].astype(F32)
    for g in range(out_ref.shape[0]):
        out_ref[g, :BS, :] = b_ref[...]
        out_ref[g, BS:, :] = jnp.where(below, cols - float(g * BS), 0.0)


def inner_products(dots_ref, vs, q, p, j):
    dots_ref[...] = jnp.zeros(dots_ref.shape, F32)
    for n in range(2):
        cut = slice(n * BS, (n + 1) * BS)
        base = n * PER_SYSTEM
        qn, pn = q[:, cut], p[:, cut]
        for i in range(j):
            vn = vs[i][:, cut]
            dots_ref[base + i : base + i + 1, :] = total(vn * pn)
            dots_ref[base + GRAM + i : base + GRAM + i + 1, :] = total(vn * qn)
        dots_ref[base + j : base + j + 1, :] = total(qn * pn)
        dots_ref[base + QQ : base + QQ + 1, :] = total(qn * qn)
        dots_ref[base + PP : base + PP + 1, :] = total(pn * pn)
    row = lax.dot_general(
        jnp.ones((8, BS), F32), dots_ref[...], (((1,), (1,)), ((), ())),
        precision=lax.Precision.HIGHEST, preferred_element_type=F32,
    )[0:1, :]
    return jnp.concatenate([row, jnp.zeros((1, BS - row.shape[1]), F32)], axis=1)


def system_row(ride, n):
    row = ride[:, :BS]
    return pltpu.roll(row, BS - n * PER_SYSTEM, 1) if n else row


def widened(row):
    return jnp.concatenate([row, jnp.zeros_like(row)], axis=1)


def arrived(got_ref, scatter_ref):
    flat = got_ref[...].reshape(-1, 2 * BS)
    return pick(scatter_ref[...], flat, 2)


def ridden(got_ref):
    slots = got_ref.shape[1]
    ride = got_ref[0, slots - 1 : slots, :]
    for s in range(1, got_ref.shape[0]):
        ride = ride + got_ref[s, slots - 1 : slots, :]
    return ride


def first_kernel(got_ref, over_ref, b_ref, diag_ref, wanted_ref, scatter_ref, p_ref, out_ref, dots_ref):
    sources, slots = got_ref.shape[0], got_ref.shape[1]
    lists = jnp.concatenate([got_ref[g, slots - 1 : slots, :BS] for g in range(sources)], axis=0).T
    lane = lax.broadcasted_iota(jnp.int32, (slots, BS), 1).astype(F32)
    rows = [jnp.where(lists[:slots, g : g + 1] == lane, 1.0, 0.0) for g in range(sources)]
    scatter_ref[...] = jnp.concatenate(rows, axis=0).T.astype(BF16)
    b = b_ref[...]
    p = arrived(got_ref, scatter_ref) + jnp.concatenate([diag_ref[...]] * 2, axis=1) * b
    p_ref[...] = p
    send_out(p, wanted_ref, widened(inner_products(dots_ref, [], b, p, 0)) + over_ref[0:1, :], out_ref)


def column_of(ride, j):
    lane = lax.broadcasted_iota(jnp.int32, (1, BS), 1)
    out = []
    for n in range(2):
        row = system_row(ride, n)
        inverse = 1.0 / jnp.sqrt(lane_of(row, QQ) + epsilon)
        h = row * jnp.where(lane == j, inverse * inverse, jnp.broadcast_to(inverse, (1, BS)))
        out.append((h, inverse))
    return out


def step_kernel(j, *refs):
    got_ref, scatter_ref, q_ref, p_ref, diag_ref, wanted_ref = refs[:6]
    v_refs = refs[6 : 6 + j]
    m_refs = refs[6 + j : 6 + 2 * j]
    v_ref, m_ref, q_out, p_out, ride_out, out_ref, dots_ref = refs[6 + 2 * j :]
    ride = ridden(got_ref)
    ride_out[...] = jnp.broadcast_to(ride, ride_out.shape)
    coeffs = column_of(ride, j)
    z = arrived(got_ref, scatter_ref)
    for n, (h, inverse) in enumerate(coeffs):
        cut = slice(n * BS, (n + 1) * BS)
        pn = p_ref[:, cut]
        v = q_ref[:, cut] * inverse
        m = pn * inverse
        v_ref[:, cut] = v
        m_ref[:, cut] = m
        q_next = m - lane_of(h, j) * v
        p_next = (z[:, cut] + diag_ref[...] * pn) * inverse - lane_of(h, j) * m
        for i in range(j):
            q_next = q_next - lane_of(h, i) * v_refs[i][:, cut]
            p_next = p_next - lane_of(h, i) * m_refs[i][:, cut]
        q_out[:, cut] = q_next
        p_out[:, cut] = p_next
    p = p_out[...]
    ride = inner_products(dots_ref, [r[...] for r in v_refs] + [v_ref[...]], q_out[...], p, j + 1)
    if j + 1 == STEPS - 1:
        out_ref[...] = jnp.broadcast_to(ride[:, None, :], out_ref.shape)
    else:
        send_out(p, wanted_ref, widened(ride), out_ref)


GRAM_AT, NUMBERS_AT = 16, 24
KEPT_ROWS = 96


def rotations_kernel(*refs):
    ride_refs, kept_ref = refs[:-1], refs[-1]
    rides = [r[0:1, :] for r in ride_refs]
    per_step = [column_of(ride, j) for j, ride in enumerate(rides)]
    lane = lax.broadcasted_iota(jnp.int32, (1, BS), 1)
    known = len(rides)
    kept_ref[...] = jnp.zeros(kept_ref.shape, F32)
    for n in range(2):
        rows = [system_row(ride, n) for ride in rides]
        norms = [jnp.sqrt(lane_of(row, QQ) + epsilon) for row in rows]
        inverses = [per_step[j][n][1] for j in range(known)]
        for j in range(known):
            column = jnp.where(lane <= j, per_step[j][n][0], 0.0)
            if j + 1 < known:
                column = jnp.where(lane == j + 1, norms[j + 1], column)
            kept_ref[n, j : j + 1, :] = column
            gram = pltpu.roll(rows[j], BS - GRAM, 1) * inverses[j]
            own = lane_of(rows[j], QQ) * inverses[j] * inverses[j]
            gram = jnp.where(lane < j, 2.0 * gram, 0.0)
            kept_ref[n, GRAM_AT + j : GRAM_AT + j + 1, :] = jnp.where(lane == j, own, gram)
        targets = [norms[0]] + [jnp.zeros_like(norms[0])] * known
        cosines, sines, triangle = [], [], []
        for j in range(known - 1):
            column = [lane_of(per_step[j][n][0], i) for i in range(j + 1)]
            rotate(column + [norms[j + 1]], cosines, sines, targets, triangle)
        numbers = cosines + sines + [x for column in triangle for x in column] + targets[:known]
        for at, number in enumerate(numbers):
            kept_ref[n, NUMBERS_AT + at : NUMBERS_AT + at + 1, :] = jnp.broadcast_to(number, (1, BS))


def finish_kernel(last_ref, kept_ref, q_ref, *refs):
    v_refs, (solution_ref, hessenberg_ref) = refs[:-2], refs[-2:]
    known = STEPS - 1
    ride = jnp.sum(last_ref[...], axis=0)
    lane = lax.broadcasted_iota(jnp.int32, (1, BS), 1)
    both = []
    for n, (h, inverse) in enumerate(column_of(ride, known)):
        row = system_row(ride, n)
        norm = jnp.sqrt(lane_of(row, QQ) + epsilon)
        h = jnp.where(lane <= known, h, 0.0)
        gram = jnp.where(lane < known, 2.0 * pltpu.roll(row, BS - GRAM, 1) * inverse, 0.0)
        gram = jnp.where(lane == known, lane_of(row, QQ) * inverse * inverse, gram)
        table = jnp.concatenate([kept_ref[n, GRAM_AT : GRAM_AT + known, :], gram], axis=0)
        column = jnp.broadcast_to(h, (8, BS)).T[:8, :1]
        form = jnp.sum(jnp.sum(table * h * column, axis=1, keepdims=True), axis=0, keepdims=True)
        twice = 2.0 * jnp.sum(h * h, axis=1, keepdims=True)
        remainder = lane_of(row, PP) * inverse * inverse - twice + form
        final_norm = jnp.sqrt(jnp.maximum(remainder, 0.0) + epsilon)
        columns = jnp.concatenate([kept_ref[n, :known, :], jnp.where(lane == known + 1, final_norm, h)], axis=0)
        before_last = lax.broadcasted_iota(jnp.int32, columns.shape, 0) == known - 1
        columns = jnp.where(before_last & (lane == known), norm, columns)
        hessenberg_ref[n] = columns.T[: STEPS + 1, :]

        def number(at):
            return kept_ref[n, NUMBERS_AT + at : NUMBERS_AT + at + 1, :]

        cosines = [number(i) for i in range(known - 1)]
        sines = [number(known - 1 + i) for i in range(known - 1)]
        at, triangle = 2 * (known - 1), []
        for j in range(known - 1):
            triangle.append([number(at + i) for i in range(j + 1)])
            at += j + 1
        targets = [number(at + i) for i in range(known)] + [None, None]
        wide = jnp.zeros((1, BS), F32)
        previous = kept_ref[n, known - 1 : known, :]
        column = [wide + lane_of(previous, i) for i in range(known)] + [wide + norm]
        rotate(column, cosines, sines, targets, triangle)
        column = [wide + lane_of(h, i) for i in range(STEPS)] + [wide + final_norm]
        rotate(column, cosines, sines, targets, triangle)
        weights = back_substitute(triangle, targets)
        cut = slice(n * BS, (n + 1) * BS)
        acc = (weights[-1] * inverse) * q_ref[:, cut]
        for i in range(STEPS - 1):
            acc = acc + weights[i] * v_refs[i][:, cut]
        both.append(acc)
    for block in range(BS):
        row = jnp.concatenate([acc[block : block + 1, :] for acc in both], axis=0)
        solution_ref[:, block * BS : (block + 1) * BS] = row


def body(blocks, block_rows, block_cols, diagonal, right_sides):
    rows_n, cols_n = lax.axis_size(ROW), lax.axis_size(COL)
    count = blocks.shape[0]
    diag = diagonal.reshape(-1, BS)
    pitch = BS + 8

    pieces_out, q = call(
        open_kernel,
        (jax.ShapeDtypeStruct((rows_n, pitch, 2 * BS), F32), jax.ShapeDtypeStruct((BS, 2 * BS), F32)),
        (right_sides, block_cols),
        name="open",
    )
    got = swap(pieces_out, ROW)
    stored = turn_blocks(blocks)
    from_whole, spread, sums, lists, over = call(
        functools.partial(plan_kernel, rows_n, cols_n),
        (
            jax.ShapeDtypeStruct((count, rows_n * pitch), BF16),
            jax.ShapeDtypeStruct((count, rows_n * SRC_SLOTS), BF16),
            jax.ShapeDtypeStruct((cols_n * DST_SLOTS, count), BF16),
            jax.ShapeDtypeStruct((8, cols_n * DST_SLOTS), F32),
            jax.ShapeDtypeStruct((8, 2 * BS), F32),
        ),
        (block_cols, block_rows),
        name="plan",
    )

    out_shape = jax.ShapeDtypeStruct((rows_n, SRC_SLOTS, 2 * BS), F32)
    vec = jax.ShapeDtypeStruct((BS, 2 * BS), F32)
    dots = pltpu.VMEM((2 * PER_SYSTEM, BS), F32)

    partial, turned, wanted = first_products(got, from_whole, stored, sums, lists)
    got = swap(partial, COL)
    scatter, p, send = call(
        first_kernel,
        (jax.ShapeDtypeStruct((BS, cols_n * DST_SLOTS), BF16), vec, out_shape),
        (got, over, q, diag, wanted),
        [dots],
        name="first",
    )
    vs, ms, rides = [], [], []
    for j in range(STEPS - 1):
        got = swap(block_products(swap(send, ROW), spread, turned, sums), COL)
        last = j + 1 == STEPS - 1
        outs = (
            vec, vec, vec, vec, jax.ShapeDtypeStruct((8, 2 * BS), F32),
            jax.ShapeDtypeStruct((rows_n * cols_n, 1, BS), F32) if last else out_shape,
        )
        v, m, q, p, ride, send = call(
            functools.partial(step_kernel, j), outs, (got, scatter, q, p, diag, wanted, *vs, *ms), [dots],
            name=f"step_{j}",
        )
        vs.append(v)
        ms.append(m)
        rides.append(ride)
    final = swap(send, BOTH)
    so_far = call(
        rotations_kernel, jax.ShapeDtypeStruct((2, KEPT_ROWS, BS), F32), tuple(rides), name="rotations"
    )

    def compact(final, so_far, q, *vs):
        solution, hessenberg = call(
            finish_kernel,
            (
                jax.ShapeDtypeStruct((2, BS * BS), F32),
                jax.ShapeDtypeStruct((2, STEPS + 1, STEPS), F32),
            ),
            (final, so_far, q, *vs),
            name="finish",
        )
        return solution, hessenberg

    return lax.cond(
        rides[0][0, FLAG] > 0.0,
        lambda *args: dense_cycle(*args[:5]),
        lambda *args: compact(*args[5:]),
        blocks, block_rows, block_cols, diagonal, right_sides, final, so_far, q, *vs,
    )


def solution(mesh):
    placed = (P(BOTH, None, None), P(BOTH, None), P(BOTH, None), P(BOTH), P(None, BOTH))
    return jax.shard_map(
        body, mesh=mesh, in_specs=placed, out_specs=(P(None, BOTH), P()), check_vma=False
    )
```
